16 devices in a mesh: dp: 4 (over z, y), tp: 4 (over x, core).
Axes of the slice: x: 2, y: 2, z: 2, core: 2. Of those that a mesh axis runs over, the one named last changes fastest.
Arguments:
- hidden: bfloat16 [128, 512, 768], P('dp')
- positions: int32 [128, 80], P('dp')
- labels: int32 [128, 80], P('dp')
- weights: float32 [128, 80], P('dp')
- w_t: bfloat16 [768, 768], replicated
- b_t: float32 [768], replicated
- gamma: float32 [768], replicated
- beta: float32 [768], replicated
- embed: bfloat16 [50304, 768], P('tp')
- out_bias: float32 [50304], P('tp')
Outputs:
- output 1: float32 [], replicated
- output 2: bfloat16 [128, 512, 768], P('dp')
- output 3: float32 [768, 768], replicated
- output 4: float32 [768], replicated
- output 5: float32 [768], replicated
- output 6: float32 [768], replicated
- output 7: float32 [50304, 768], P('tp')
- output 8: float32 [50304], P('tp')
All inputs are finite; a program needn't handle non-finite values.
Results may differ from the reference program's by a relative error of at most 0.001.
Values sent between devices are 32-bit elements.
A program may use at most 1 GiB of HBM per device.

```python
import jax
import jax.numpy as jnp
from jax import lax

HIDDEN = 768
VOCAB_REAL = 50265
VOCAB_PAD = 50304
SEQ_LEN = 512
MAX_PRED = 80
BATCH_TOTAL = 128
BLOCK_SEQ = 8
NUM_BLOCKS = BATCH_TOTAL // BLOCK_SEQ
BLOCK_ROWS = BLOCK_SEQ * MAX_PRED
LN_EPS = 1e-12
LOSS_EPS = 1e-5


def setup_inputs(seed: int = 0) -> dict:
    key = jax.random.key(seed)
    keys = jax.random.split(key, 10)
    hidden = jax.random.normal(keys[0], (BATCH_TOTAL, SEQ_LEN, HIDDEN), jnp.float32).astype(jnp.bfloat16)
    row_keys = jax.random.split(keys[1], BATCH_TOTAL)
    positions = jax.vmap(lambda row_key: jax.random.permutation(row_key, SEQ_LEN)[:MAX_PRED])(row_keys).astype(jnp.int32)
    labels = jax.random.randint(keys[2], (BATCH_TOTAL, MAX_PRED), 0, VOCAB_REAL, dtype=jnp.int32)
    pred_counts = jax.random.randint(keys[3], (BATCH_TOTAL,), 1, MAX_PRED + 1, dtype=jnp.int32).at[0].set(MAX_PRED)
    weights = (jnp.arange(MAX_PRED, dtype=jnp.int32)[None, :] < pred_counts[:, None]).astype(jnp.float32)
    w_t = (jax.random.normal(keys[4], (HIDDEN, HIDDEN), jnp.float32) * HIDDEN ** -0.5).astype(jnp.bfloat16)
    b_t = 0.5 * jax.random.normal(keys[5], (HIDDEN,), jnp.float32)
    gamma = 1.0 + 0.3 * jax.random.normal(keys[6], (HIDDEN,), jnp.float32)
    beta = 0.3 * jax.random.normal(keys[7], (HIDDEN,), jnp.float32)
    embed = (jax.random.normal(keys[8], (VOCAB_PAD, HIDDEN), jnp.float32) * (1.5 * HIDDEN ** -0.5)).astype(jnp.bfloat16)
    raw_bias = 0.5 * jax.random.normal(keys[9], (VOCAB_PAD,), jnp.float32)
    out_bias = jnp.where(jnp.arange(VOCAB_PAD) < VOCAB_REAL, raw_bias, -1e9)
    return {"hidden": hidden, "positions": positions, "labels": labels, "weights": weights, "w_t": w_t, "b_t": b_t, "gamma": gamma, "beta": beta, "embed": embed, "out_bias": out_bias}


def gelu_norm(pre_act, gamma, beta):
    activated = jax.nn.gelu(pre_act, approximate=False)
    mean_val = jnp.mean(activated, axis=-1, keepdims=True)
    centered = activated - mean_val
    variance = jnp.mean(centered * centered, axis=-1, keepdims=True)
    return centered * lax.rsqrt(variance + LN_EPS) * gamma + beta


def reference(hidden, positions, labels, weights, w_t, b_t, gamma, beta, embed, out_bias):
    picked = jnp.take_along_axis(hidden, positions[:, :, None], axis=1)
    tok_rows = picked.reshape(BATCH_TOTAL * MAX_PRED, HIDDEN)
    pre_act = jnp.dot(tok_rows, w_t, preferred_element_type=jnp.float32) + b_t
    normed, norm_vjp = jax.vjp(gelu_norm, pre_act, gamma, beta)
    t_bf = normed.astype(jnp.bfloat16)
    flat_w = weights.reshape(-1)
    denom = jnp.sum(flat_w) + LOSS_EPS
    vocab_ids = jnp.arange(VOCAB_PAD, dtype=jnp.int32)

    def block_step(carry, block):
        d_embed, d_bias, loss_sum = carry
        t_blk, lab_blk, w_blk = block
        logits = jnp.dot(t_blk, embed.T, preferred_element_type=jnp.float32) + out_bias
        row_max = jnp.max(logits, axis=1)
        shifted = jnp.exp(logits - row_max[:, None])
        sum_exp = jnp.sum(shifted, axis=1)
        log_norm = jnp.log(sum_exp) + row_max
        lab_hot = lab_blk[:, None] == vocab_ids[None, :]
        target_logit = jnp.sum(jnp.where(lab_hot, logits, 0.0), axis=1)
        soft_probs = shifted * (1.0 / sum_exp)[:, None]
        d_logits = jnp.where(lab_hot, soft_probs - 1.0, soft_probs) * (w_blk / denom)[:, None]
        dz_bf = d_logits.astype(jnp.bfloat16)
        d_embed = d_embed + jnp.dot(dz_bf.T, t_blk, preferred_element_type=jnp.float32)
        d_bias = d_bias + jnp.sum(d_logits, axis=0)
        loss_sum = loss_sum + jnp.sum(w_blk * (log_norm - target_logit))
        d_normed = jnp.dot(dz_bf, embed, preferred_element_type=jnp.float32)
        return (d_embed, d_bias, loss_sum), d_normed

    init = (jnp.zeros((VOCAB_PAD, HIDDEN), jnp.float32), jnp.zeros((VOCAB_PAD,), jnp.float32), jnp.zeros((), jnp.float32))
    blocks = (t_bf.reshape(NUM_BLOCKS, BLOCK_ROWS, HIDDEN), labels.reshape(NUM_BLOCKS, BLOCK_ROWS), flat_w.reshape(NUM_BLOCKS, BLOCK_ROWS))
    (d_embed, d_out_bias, loss_sum), d_normed = lax.scan(block_step, init, blocks)
    loss = loss_sum / denom
    d_pre, d_gamma, d_beta = norm_vjp(d_normed.reshape(BATCH_TOTAL * MAX_PRED, HIDDEN))
    d_pre_bf = d_pre.astype(jnp.bfloat16)
    d_w_t = jnp.dot(tok_rows.T, d_pre_bf, preferred_element_type=jnp.float32)
    d_b_t = jnp.sum(d_pre, axis=0)
    d_rows = jnp.dot(d_pre_bf, w_t.T, preferred_element_type=jnp.float32).astype(jnp.bfloat16)
    row_ids = jnp.arange(BATCH_TOTAL)[:, None]
    d_hidden = jnp.zeros((BATCH_TOTAL, SEQ_LEN, HIDDEN), jnp.bfloat16).at[row_ids, positions].add(d_rows.reshape(BATCH_TOTAL, MAX_PRED, HIDDEN))
    return (loss, d_hidden, d_w_t, d_b_t, d_gamma, d_beta, d_embed, d_out_bias)
```

```python
import functools

import jax
import jax.numpy as jnp
from jax import lax
from jax.experimental import pallas as pl
from jax.experimental.pallas import tpu as pltpu
from jax.sharding import PartitionSpec as P

LN_EPS = 1e-12
LOSS_EPS = 1e-5
VOCAB_BLOCKS = 6
TOK = 256
CHUNK = 256
STAGES = 4
PICK = 96
OFF = 1e30
VMEM_LIMIT = 67_000_000


def gelu_norm(pre_act, gamma, beta):
    activated = jax.nn.gelu(pre_act, approximate=False)
    mean_val = jnp.mean(activated, axis=-1, keepdims=True)
    centered = activated - mean_val
    variance = jnp.mean(centered * centered, axis=-1, keepdims=True)
    return centered * lax.rsqrt(variance + LN_EPS) * gamma + beta


def dot_nt(a, b):
    return lax.dot_general(a, b, (((1,), (1,)), ((), ())), preferred_element_type=jnp.float32)


def dot_tn(a, b):
    return lax.dot_general(a, b, (((0,), (0,)), ((), ())), preferred_element_type=jnp.float32)


def dot_nn(a, b):
    return jnp.dot(a, b, preferred_element_type=jnp.float32)


def hot_rows(row, seq_len):
    ids = lax.broadcasted_iota(jnp.int32, (seq_len, PICK), 0)
    return jnp.where(ids == row[:, :PICK], 1.0, 0.0).astype(jnp.bfloat16)


def pick_kernel(base_ref, idx_ref, hidden_ref, out_ref, acc):
    seq = pl.program_id(0)

    @pl.when(seq == 0)
    def _():
        acc[...] = jnp.zeros_like(acc)

    rows = dot_tn(hot_rows(idx_ref[0], hidden_ref.shape[1]), hidden_ref[0])
    base = pl.multiple_of(base_ref[seq], 8)
    acc[pl.ds(base, 16), :] += rows[:16]
    acc[pl.ds(base + 16, PICK - 16), :] = rows[16:]

    @pl.when(seq == pl.num_programs(0) - 1)
    def _():
        out_ref[...] = acc[...].astype(jnp.bfloat16)


def place_kernel(base_ref, idx_ref, rows_ref, out_ref):
    seq = pl.program_id(0)
    base = pl.multiple_of(base_ref[seq], 8)
    rows = rows_ref[pl.ds(base, PICK), :].astype(jnp.bfloat16)
    out_ref[0] = dot_nn(hot_rows(idx_ref[0], out_ref.shape[1]), rows).astype(jnp.bfloat16)


def for_blocks(count, body):
    def pair(step, carry):
        body(2 * step, 0)
        body(2 * step + 1, 1)
        return carry

    lax.fori_loop(0, count // 2, pair, 0)

    @pl.when(count % 2 == 1)
    def _():
        body(count - 1, 0)


def tile_bias(bias_ref):
    bias = bias_ref[...]
    return jnp.concatenate([bias] * (TOK // bias.shape[1]), axis=1)


def stats_kernel(count_ref, lab_ref, tok_ref, embed_ref, bias_ref, out_ref, z0, z1):
    vblk = pl.program_id(0)
    height = embed_ref.shape[0]

    @pl.when(vblk == 0)
    def _():
        out_ref[...] = jnp.zeros_like(out_ref)
        out_ref[0:1, :] = jnp.full((1, out_ref.shape[1]), -jnp.inf, jnp.float32)

    def body(block, slot):
        z_ref = (z0, z1)[slot]
        cols = pl.ds(pl.multiple_of(block * TOK, TOK), TOK)
        z_ref[...] = dot_nt(embed_ref[...], tok_ref[cols, :]) + tile_bias(bias_ref)
        old_max = out_ref[0:1, cols]
        new_max = jnp.maximum(old_max, jnp.max(z_ref[...], axis=0, keepdims=True))
        part = jnp.sum(jnp.exp(z_ref[...] - new_max), axis=0, keepdims=True)
        ids = lax.broadcasted_iota(jnp.int32, (height, TOK), 0)
        hit = ids == lab_ref[0:1, cols] - vblk * height
        target = jnp.sum(jnp.where(hit, z_ref[...], 0.0), axis=0, keepdims=True)
        out_ref[1:2, cols] = out_ref[1:2, cols] * jnp.exp(old_max - new_max) + part
        out_ref[0:1, cols] = new_max
        out_ref[2:3, cols] += target

    for_blocks(count_ref[0], body)


def logit_grad(vblk, block, tok, lab_ref, meta_ref, embed_ref, bias_ref, dbias_ref, z_ref, dz_ref):
    cols = pl.ds(pl.multiple_of(block * TOK, TOK), TOK)
    height = embed_ref.shape[0]
    z_ref[...] = dot_nt(embed_ref[...], tok)
    ids = lax.broadcasted_iota(jnp.int32, (height, TOK), 0)
    hit = ids == lab_ref[0:1, cols] - vblk * height
    probs = jnp.exp(z_ref[...] + tile_bias(bias_ref) - meta_ref[0:1, cols]) * meta_ref[1:2, cols]
    dz = probs - jnp.where(hit, meta_ref[2:3, cols], 0.0)
    lanes = dbias_ref.shape[1]
    part = dz[:, :lanes]
    for k in range(1, TOK // lanes):
        part = part + dz[:, k * lanes:(k + 1) * lanes]
    dbias_ref[...] += part
    dz_ref[...] = dz.astype(jnp.bfloat16)


def own_kernel(count_ref, lab_ref, meta_ref, tok_ref, embed_ref, bias_ref, dembed_ref, dbias_ref, dtok_ref, z0, z1, dz0, dz1):
    vblk = pl.program_id(0)

    @pl.when(vblk == 0)
    def _():
        dtok_ref[...] = jnp.zeros_like(dtok_ref)

    dembed_ref[...] = jnp.zeros_like(dembed_ref)
    dbias_ref[...] = jnp.zeros_like(dbias_ref)

    def body(block, slot):
        z_ref, dz_ref = (z0, z1)[slot], (dz0, dz1)[slot]
        rows = pl.ds(pl.multiple_of(block * TOK, TOK), TOK)
        tok = tok_ref[rows, :]
        logit_grad(vblk, block, tok, lab_ref, meta_ref, embed_ref, bias_ref, dbias_ref, z_ref, dz_ref)
        dembed_ref[...] += dot_nn(dz_ref[...], tok)
        dtok_ref[rows, :] += dot_tn(dz_ref[...], embed_ref[...])

    for_blocks(count_ref[0], body)


def rest_kernel(plan_ref, src_ref, dst_ref, lab_ref, meta_ref, embed_ref, bias_ref, dembed_in_ref, tok_hbm, dembed_ref, dbias_ref, tok_ref, stage, sems, z0, z1, dz0, dz1):
    vblk = pl.program_id(0)
    chunks = plan_ref[1]

    def fetch(chunk):
        slot = lax.rem(chunk, STAGES)
        src = tok_hbm.at[pl.ds(pl.multiple_of(src_ref[chunk], CHUNK), CHUNK), :]
        return pltpu.make_async_copy(src, stage.at[slot], sems.at[slot])

    @pl.when(vblk == 0)
    def _():
        end = pl.multiple_of(plan_ref[2], 16)
        tok_ref[pl.ds(end, TOK), :] = jnp.zeros((TOK, tok_ref.shape[1]), jnp.bfloat16)
        for first in range(STAGES):
            @pl.when(first < chunks)
            def _():
                fetch(first).start()

        def take(chunk, carry):
            fetch(chunk).wait()
            dst = pl.multiple_of(dst_ref[chunk], 16)
            tok_ref[pl.ds(dst, CHUNK), :] = stage[lax.rem(chunk, STAGES)].astype(jnp.bfloat16)

            @pl.when(chunk + STAGES < chunks)
            def _():
                fetch(chunk + STAGES).start()
            return carry

        lax.fori_loop(0, chunks, take, 0)

    dembed_ref[...] = dembed_in_ref[...]
    dbias_ref[...] = jnp.zeros_like(dbias_ref)

    def body(block, slot):
        z_ref, dz_ref = (z0, z1)[slot], (dz0, dz1)[slot]
        tok = tok_ref[pl.ds(pl.multiple_of(block * TOK, TOK), TOK), :]
        logit_grad(vblk, block, tok, lab_ref, meta_ref, embed_ref, bias_ref, dbias_ref, z_ref, dz_ref)
        dembed_ref[...] += dot_nn(dz_ref[...], tok)

    for_blocks(plan_ref[0], body)


def whole(shape):
    return pl.BlockSpec(shape, lambda *_: (0,) * len(shape))


def by_rows(shape):
    return pl.BlockSpec(shape, lambda step, *_: (step,) + (0,) * (len(shape) - 1))


def run(kernel, scalars, grid, args, in_specs, out_specs, out_shape, scratch, flops, aliases=None):
    return pl.pallas_call(
        kernel,
        grid_spec=pltpu.PrefetchScalarGridSpec(
            num_scalar_prefetch=len(scalars), grid=(grid,), in_specs=in_specs, out_specs=out_specs, scratch_shapes=scratch
        ),
        out_shape=out_shape,
        input_output_aliases=aliases or {},
        compiler_params=pltpu.CompilerParams(dimension_semantics=("arbitrary",), vmem_limit_bytes=VMEM_LIMIT),
        cost_estimate=pl.CostEstimate(flops=flops, bytes_accessed=40_000_000, transcendentals=0),
    )(*scalars, *args)


def solution(mesh):
    groups, shards = mesh.shape["dp"], mesh.shape["tp"]
    f32, bf16, i32 = jnp.float32, jnp.bfloat16, jnp.int32

    def local_step(hidden, positions, labels, weights, w_t, b_t, gamma, beta, embed, out_bias):
        batch, seq_len, width = hidden.shape
        max_pred = positions.shape[1]
        rows = batch * max_pred
        vocab = embed.shape[0]
        height = vocab // VOCAB_BLOCKS
        me_dp, me_tp = lax.axis_index("dp"), lax.axis_index("tp")

        live = jnp.sum(weights, axis=1).astype(i32)
        seqs = jnp.arange(batch, dtype=i32)
        offset = jnp.sum(jnp.where(seqs[None, :] < seqs[:, None], live[None, :], 0), axis=1)
        base = jnp.minimum(offset // 8 * 8, rows - PICK)
        slots = jnp.arange(max_pred, dtype=i32)
        alive = slots[None, :] < live[:, None]
        place = jnp.where(alive, slots[None, :] + (offset - base)[:, None], -1)
        lanes = jnp.arange(128, dtype=i32)
        idx_rows = jnp.sum(jnp.where(place[:, None, :] == lanes[None, :, None], positions[:, None, :] + 1, 0), axis=2) - 1
        idx_rows = idx_rows.reshape(batch, 1, 128)
        packed = jnp.where(alive, slots[None, :] + offset[:, None], -1).reshape(-1)
        lab = jnp.sum(jnp.where(packed[None, :] == jnp.arange(rows, dtype=i32)[:, None], labels.reshape(-1)[None, :] + 1, 0), axis=1) - 1
        count = jnp.sum(live)
        blocks = ((count + TOK - 1) // TOK).reshape(1)

        picked = run(
            pick_kernel, (base,), batch, (idx_rows, hidden),
            [by_rows((1, 1, 128)), by_rows((1, seq_len, width))], whole((rows, width)),
            jax.ShapeDtypeStruct((rows, width), bf16), [pltpu.VMEM((rows, width), f32)], 8_000_000_000,
        )
        pre_act = jnp.dot(picked, w_t, preferred_element_type=f32) + b_t
        normed, norm_vjp = jax.vjp(gelu_norm, pre_act, gamma, beta)
        tok = normed.astype(bf16)
        share = rows // shards
        mine = lax.dynamic_slice(normed, (me_tp * share, 0), (share, width))
        tok_all = lax.all_gather(mine, ("dp", "tp"), tiled=True)

        bias = jnp.broadcast_to(out_bias[:, None], (vocab, 128))
        local_lab = jnp.where(lab >= 0, lab - me_tp * vocab, -1)
        z_scratch = [pltpu.VMEM((height, TOK), f32)] * 2
        dz_scratch = [pltpu.VMEM((height, TOK), bf16)] * 2
        stats = run(
            stats_kernel, (blocks,), VOCAB_BLOCKS, (local_lab[None, :], tok, embed, bias),
            [whole((1, rows)), whole((rows, width)), by_rows((height, width)), by_rows((height, 128))], whole((8, rows)),
            jax.ShapeDtypeStruct((8, rows), f32), z_scratch, 25_000_000_000,
        )
        packet = jnp.concatenate([stats[:3], lab.astype(f32)[None, :]], axis=0)
        packets = lax.all_gather(packet, ("dp", "tp")).reshape(groups, shards, 4, rows)
        labs = packets[:, 0, 3, :].astype(i32)
        valid = labs >= 0
        maxes = jnp.where(valid[:, None, :], packets[:, :, 0, :], 0.0)
        row_max = jnp.max(maxes, axis=1)
        sum_exp = jnp.where(valid, jnp.sum(packets[:, :, 1, :] * jnp.exp(maxes - row_max[:, None, :]), axis=1), 1.0)
        target = jnp.sum(packets[:, :, 2, :], axis=1)
        lives = jnp.sum(valid, axis=1).astype(i32)
        denom = jnp.sum(lives).astype(f32) + LOSS_EPS
        loss = jnp.sum(jnp.where(valid, jnp.log(sum_exp) + row_max - target, 0.0)) / denom
        inv = 1.0 / denom
        metas = jnp.stack([
            jnp.where(valid, row_max, OFF),
            jnp.where(valid, (1.0 / sum_exp) * inv, 0.0),
            jnp.where(valid, inv, 0.0),
            jnp.where(valid, labs - me_tp * vocab, -1).astype(f32),
        ], axis=1)

        own_meta = lax.dynamic_index_in_dim(metas, me_dp, 0, keepdims=False)
        d_embed, d_bias_own, d_tok = run(
            own_kernel, (blocks,), VOCAB_BLOCKS, (local_lab[None, :], own_meta, tok, embed, bias),
            [whole((1, rows)), whole((4, rows)), whole((rows, width)), by_rows((height, width)), by_rows((height, 128))],
            [by_rows((height, width)), by_rows((height, 128)), whole((rows, width))],
            [jax.ShapeDtypeStruct((vocab, width), f32), jax.ShapeDtypeStruct((vocab, 128), f32), jax.ShapeDtypeStruct((rows, width), f32)],
            z_scratch + dz_scratch, 75_000_000_000,
        )
        d_normed = lax.psum(d_tok, "tp")

        cap = (groups - 1) * rows
        meta = jnp.concatenate([jnp.full((1, cap + TOK), OFF, f32), jnp.zeros((2, cap + TOK), f32), jnp.full((1, cap + TOK), -1.0, f32)], axis=0)
        pos = jnp.int32(0)
        ids = jnp.arange(cap // CHUNK, dtype=i32)
        src, dst, chunks = jnp.zeros_like(ids), jnp.zeros_like(ids), jnp.int32(0)
        for k in range(1, groups):
            peer = lax.rem(me_dp + k, groups)
            meta = lax.dynamic_update_slice(meta, lax.dynamic_index_in_dim(metas, peer, 0, keepdims=False), (0, pos))
            size = lax.dynamic_index_in_dim(lives, peer, 0, keepdims=False)
            parts = (size + CHUNK - 1) // CHUNK
            inside = ids >= chunks
            src = jnp.where(inside, peer * rows + (ids - chunks) * CHUNK, src)
            dst = jnp.where(inside, pos + (ids - chunks) * CHUNK, dst)
            chunks = chunks + parts
            last = pos + parts * CHUNK
            pos = pos + (size + 15) // 16 * 16
        plan = jnp.stack([(pos + TOK - 1) // TOK, chunks, last])
        meta_lab = meta[3:4].astype(i32)
        d_embed, d_bias_rest = run(
            rest_kernel, (plan, src, dst), VOCAB_BLOCKS, (meta_lab, meta, embed, bias, d_embed, tok_all),
            [whole((1, cap + TOK)), whole((4, cap + TOK)), by_rows((height, width)), by_rows((height, 128)), by_rows((height, width)), pl.BlockSpec(memory_space=pl.ANY)],
            [by_rows((height, width)), by_rows((height, 128))],
            [jax.ShapeDtypeStruct((vocab, width), f32), jax.ShapeDtypeStruct((vocab, 128), f32)],
            [pltpu.VMEM((cap + TOK, width), bf16), pltpu.VMEM((STAGES, CHUNK, width), f32), pltpu.SemaphoreType.DMA((STAGES,))] + z_scratch + dz_scratch,
            150_000_000_000, {7: 0},
        )
        d_out_bias = jnp.sum(d_bias_own + d_bias_rest, axis=1)

        d_pre, d_gamma, d_beta = norm_vjp(d_normed)
        d_pre_bf = d_pre.astype(bf16)
        d_w_t = jnp.einsum("nd,ne->de", picked, d_pre_bf, preferred_element_type=f32)
        d_b_t = jnp.sum(d_pre, axis=0)
        d_w_t, d_b_t, d_gamma, d_beta = lax.psum((d_w_t, d_b_t, d_gamma, d_beta), "dp")
        d_rows = jnp.einsum("ne,de->nd", d_pre_bf, w_t, preferred_element_type=f32)
        d_hidden = run(
            place_kernel, (base,), batch, (idx_rows, d_rows),
            [by_rows((1, 1, 128)), whole((rows, width))], by_rows((1, seq_len, width)),
            jax.ShapeDtypeStruct((batch, seq_len, width), bf16), [], 8_000_000_000,
        )
        return loss, d_hidden, d_w_t, d_b_t, d_gamma, d_beta, d_embed, d_out_bias

    in_specs = (P("dp", None, None), P("dp", None), P("dp", None), P("dp", None), P(None, None), P(None), P(None), P(None), P("tp", None), P("tp"))
    out_specs = (P(), P("dp", None, None), P(None, None), P(None), P(None), P(None), P("tp", None), P("tp"))
    return jax.shard_map(local_step, mesh=mesh, in_specs=in_specs, out_specs=out_specs, check_vma=False)
```

```python
import functools

import jax
import jax.numpy as jnp
from jax import lax
from jax.experimental import pallas as pl
from jax.experimental.pallas import tpu as pltpu
from jax.sharding import PartitionSpec as P


LN_EPS = 1e-12
LOSS_EPS = 1e-5
VOCAB_BLOCKS = 6
TOK = 256
CHUNK = 256
STAGES = 4
PICK = 96
SEQS = 4
SPLIT = 4
OFF = 1e30
VMEM_LIMIT = 67_000_000


def gelu_norm(pre_act, gamma, beta):
    activated = jax.nn.gelu(pre_act, approximate=False)
    mean_val = jnp.mean(activated, axis=-1, keepdims=True)
    centered = activated - mean_val
    variance = jnp.mean(centered * centered, axis=-1, keepdims=True)
    return centered * lax.rsqrt(variance + LN_EPS) * gamma + beta


def dot_nt(a, b):
    return lax.dot_general(a, b, (((1,), (1,)), ((), ())), preferred_element_type=jnp.float32)


def dot_tn(a, b):
    return lax.dot_general(a, b, (((0,), (0,)), ((), ())), preferred_element_type=jnp.float32)


def dot_nn(a, b):
    return jnp.dot(a, b, preferred_element_type=jnp.float32)


def hot_rows(row, seq_len):
    ids = lax.broadcasted_iota(jnp.int32, (seq_len, PICK), 0)
    return jnp.where(ids == row[:, :PICK], 1.0, 0.0).astype(jnp.bfloat16)


def pick_kernel(base_ref, idx_ref, hidden_ref, out_ref, acc):
    step = pl.program_id(0)

    @pl.when(step == 0)
    def _():
        acc[...] = jnp.zeros_like(acc)

    picked = [dot_tn(hot_rows(idx_ref[k], hidden_ref.shape[1]), hidden_ref[k]) for k in range(SEQS)]
    for k, rows in enumerate(picked):
        base = pl.multiple_of(base_ref[step * SEQS + k], 8)
        acc[pl.ds(base, 16), :] += rows[:16]
        acc[pl.ds(base + 16, PICK - 16), :] = rows[16:]

    @pl.when(step == pl.num_programs(0) - 1)
    def _():
        out_ref[...] = acc[...].astype(jnp.bfloat16)


def place_kernel(base_ref, idx_ref, rows_ref, out_ref):
    step = pl.program_id(0)
    for k in range(SEQS):
        base = pl.multiple_of(base_ref[step * SEQS + k], 8)
        rows = rows_ref[pl.ds(base, PICK), :].astype(jnp.bfloat16)
        out_ref[k] = dot_nn(hot_rows(idx_ref[k], out_ref.shape[1]), rows).astype(jnp.bfloat16)


def for_blocks(count, body):
    def pair(step, carry):
        body(pl.multiple_of(step * 2 * TOK, 2 * TOK), 2 * TOK)
        return carry

    lax.fori_loop(0, count // 2, pair, 0)

    @pl.when(count % 2 == 1)
    def _():
        body(pl.multiple_of((count - 1) * TOK, TOK), TOK)


def strips(height):
    size = (height // 4 + 15) // 16 * 16
    return [(at, min(size, height - at)) for at in range(0, height, size)]


def tile_bias(bias_ref, at, size, width):
    bias = bias_ref[at:at + size, :]
    return jnp.concatenate([bias] * (width // bias.shape[1]), axis=1)


def stats_kernel(count_ref, lab_ref, tok_ref, embed_ref, bias_ref, out_ref, z_ref):
    vblk = pl.program_id(0)
    height = embed_ref.shape[0]

    @pl.when(vblk == 0)
    def _():
        out_ref[...] = jnp.zeros_like(out_ref)
        out_ref[0:1, :] = jnp.full((1, out_ref.shape[1]), -jnp.inf, jnp.float32)

    def body(start, width):
        cols = pl.ds(start, width)
        tok = tok_ref[cols, :]
        lab = lab_ref[0:1, cols] - vblk * height
        parts = []
        target = jnp.zeros((1, width), jnp.float32)
        for at, size in strips(height):
            z_ref[at:at + size, :width] = dot_nt(embed_ref[at:at + size, :], tok) + tile_bias(bias_ref, at, size, width)
        for at, size in strips(height):
            top = jnp.max(z_ref[at:at + size, :width], axis=0, keepdims=True)
            total = jnp.sum(jnp.exp(z_ref[at:at + size, :width] - top), axis=0, keepdims=True)
            hit = lax.broadcasted_iota(jnp.int32, (size, width), 0) == lab - at
            target += jnp.sum(jnp.where(hit, z_ref[at:at + size, :width], 0.0), axis=0, keepdims=True)
            parts.append((top, total))
        old_max = out_ref[0:1, cols]
        new_max = functools.reduce(jnp.maximum, [top for top, _ in parts], old_max)
        total = out_ref[1:2, cols] * jnp.exp(old_max - new_max)
        for top, part in parts:
            total += part * jnp.exp(top - new_max)
        out_ref[0:1, cols] = new_max
        out_ref[1:2, cols] = total
        out_ref[2:3, cols] += target

    for_blocks(count_ref[0], body)


def logit_grad(vblk, start, width, tok_ref, lab_ref, meta_ref, embed_ref, bias_ref, dembed_ref, dbias_ref, z_ref, dz_ref):
    cols = pl.ds(start, width)
    height, lanes = embed_ref.shape[0], dbias_ref.shape[1]
    tok = tok_ref[cols, :]
    lab = lab_ref[0:1, cols] - vblk * height
    top, scale, unit = meta_ref[0:1, cols], meta_ref[1:2, cols], meta_ref[2:3, cols]
    todo = strips(height)

    def logits(strip):
        at, size = strip
        z_ref[at:at + size, :width] = dot_nt(embed_ref[at:at + size, :], tok)

    logits(todo[0])
    for k, (at, size) in enumerate(todo):
        if k + 1 < len(todo):
            logits(todo[k + 1])
        hit = lax.broadcasted_iota(jnp.int32, (size, width), 0) == lab - at
        probs = jnp.exp(z_ref[at:at + size, :width] + tile_bias(bias_ref, at, size, width) - top) * scale
        dz = probs - jnp.where(hit, unit, 0.0)
        part = dz[:, :lanes]
        for j in range(1, width // lanes):
            part = part + dz[:, j * lanes:(j + 1) * lanes]
        dbias_ref[at:at + size, :] += part
        dz_ref[at:at + size, :width] = dz.astype(jnp.bfloat16)
        dembed_ref[at:at + size, :] += dot_nn(dz_ref[at:at + size, :width], tok)


def own_kernel(count_ref, lab_ref, meta_ref, tok_ref, embed_ref, bias_ref, dembed_ref, dbias_ref, dtok_ref, z_ref, dz_ref):
    vblk = pl.program_id(0)

    @pl.when(vblk == 0)
    def _():
        dtok_ref[...] = jnp.zeros_like(dtok_ref)

    dembed_ref[...] = jnp.zeros_like(dembed_ref)
    dbias_ref[...] = jnp.zeros_like(dbias_ref)

    def body(start, width):
        logit_grad(vblk, start, width, tok_ref, lab_ref, meta_ref, embed_ref, bias_ref, dembed_ref, dbias_ref, z_ref, dz_ref)
        dtok_ref[pl.ds(start, width), :] += dot_tn(dz_ref[:, :width], embed_ref[...])

    for_blocks(count_ref[0], body)


def rest_kernel(first, plan_ref, src_ref, dst_ref, lab_ref, meta_ref, embed_ref, bias_ref, dembed_in_ref, dbias_in_ref, tok_hbm, dembed_ref, dbias_ref, tok_ref, stage, sems, z_ref, dz_ref):
    vblk = pl.program_id(0)
    chunks = plan_ref[1]

    def fetch(chunk):
        slot = lax.rem(chunk, STAGES)
        src = tok_hbm.at[pl.ds(pl.multiple_of(src_ref[chunk], CHUNK), CHUNK), :]
        return pltpu.make_async_copy(src, stage.at[slot], sems.at[slot])

    @pl.when(vblk == 0)
    def _():
        end = pl.multiple_of(plan_ref[2], 16)
        tok_ref[pl.ds(end, TOK), :] = jnp.zeros((TOK, tok_ref.shape[1]), jnp.bfloat16)
        for k in range(STAGES):
            @pl.when(k < chunks)
            def _():
                fetch(k).start()

        def take(chunk, carry):
            fetch(chunk).wait()
            dst = pl.multiple_of(dst_ref[chunk], 16)
            tok_ref[pl.ds(dst, CHUNK), :] = stage[lax.rem(chunk, STAGES)].astype(jnp.bfloat16)

            @pl.when(chunk + STAGES < chunks)
            def _():
                fetch(chunk + STAGES).start()

            return carry

        lax.fori_loop(0, chunks, take, 0)

    dembed_ref[...] = dembed_in_ref[...]
    dbias_ref[...] = dbias_in_ref[...]

    def body(start, width):
        logit_grad(vblk + first, start, width, tok_ref, lab_ref, meta_ref, embed_ref, bias_ref, dembed_ref, dbias_ref, z_ref, dz_ref)

    for_blocks(plan_ref[0], body)


def whole(shape):
    return pl.BlockSpec(shape, lambda *_: (0,) * len(shape))


def by_rows(shape, first=0):
    return pl.BlockSpec(shape, lambda step, *_: (step + first,) + (0,) * (len(shape) - 1))


def run(kernel, scalars, grid, args, in_specs, out_specs, out_shape, scratch, flops, aliases=None):
    return pl.pallas_call(
        kernel,
        grid_spec=pltpu.PrefetchScalarGridSpec(
            num_scalar_prefetch=len(scalars), grid=(grid,), in_specs=in_specs, out_specs=out_specs, scratch_shapes=scratch
        ),
        out_shape=out_shape,
        input_output_aliases=aliases or {},
        compiler_params=pltpu.CompilerParams(dimension_semantics=("arbitrary",), vmem_limit_bytes=VMEM_LIMIT),
        cost_estimate=pl.CostEstimate(flops=flops, bytes_accessed=40_000_000, transcendentals=0),
    )(*scalars, *args)


def solution(mesh):
    groups, shards = mesh.shape["dp"], mesh.shape["tp"]
    f32, bf16, i32 = jnp.float32, jnp.bfloat16, jnp.int32

    def local_step(hidden, positions, labels, weights, w_t, b_t, gamma, beta, embed, out_bias):
        batch, seq_len, width = hidden.shape
        max_pred = positions.shape[1]
        rows = batch * max_pred
        vocab = embed.shape[0]
        height = vocab // VOCAB_BLOCKS
        me_dp, me_tp = lax.axis_index("dp"), lax.axis_index("tp")

        live = jnp.sum(weights, axis=1).astype(i32)
        seqs = jnp.arange(batch, dtype=i32)
        offset = jnp.sum(jnp.where(seqs[None, :] < seqs[:, None], live[None, :], 0), axis=1)
        base = jnp.minimum(offset // 8 * 8, rows - PICK)
        slots = jnp.arange(max_pred, dtype=i32)
        alive = slots[None, :] < live[:, None]
        place = jnp.where(alive, slots[None, :] + (offset - base)[:, None], -1)
        lanes = jnp.arange(128, dtype=i32)
        idx_rows = jnp.sum(jnp.where(place[:, None, :] == lanes[None, :, None], positions[:, None, :] + 1, 0), axis=2) - 1
        idx_rows = idx_rows.reshape(batch, 1, 128)
        packed = jnp.where(alive, slots[None, :] + offset[:, None], -1).reshape(-1)
        lab = jnp.sum(jnp.where(packed[None, :] == jnp.arange(rows, dtype=i32)[:, None], labels.reshape(-1)[None, :] + 1, 0), axis=1) - 1
        count = jnp.sum(live)
        blocks = ((count + TOK - 1) // TOK).reshape(1)

        picked = run(
            pick_kernel, (base,), batch // SEQS, (idx_rows, hidden),
            [by_rows((SEQS, 1, 128)), by_rows((SEQS, seq_len, width))], whole((rows, width)),
            jax.ShapeDtypeStruct((rows, width), bf16), [pltpu.VMEM((rows, width), f32)], 8_000_000_000,
        )
        pre_act = jnp.dot(picked, w_t, preferred_element_type=f32) + b_t
        normed, norm_vjp = jax.vjp(gelu_norm, pre_act, gamma, beta)
        tok = normed.astype(bf16)
        share = rows // shards
        mine = lax.dynamic_slice(normed, (me_tp * share, 0), (share, width))
        tok_all = lax.all_gather(mine, ("dp", "tp"), tiled=True)

        bias = jnp.broadcast_to(out_bias[:, None], (vocab, 128))
        local_lab = jnp.where(lab >= 0, lab - me_tp * vocab, -1)
        z_scratch = [pltpu.VMEM((height, 2 * TOK), f32)]
        dz_scratch = [pltpu.VMEM((height, 2 * TOK), bf16)]
        stats = run(
            stats_kernel, (blocks,), VOCAB_BLOCKS, (local_lab[None, :], tok, embed, bias),
            [whole((1, rows)), whole((rows, width)), by_rows((height, width)), by_rows((height, 128))], whole((8, rows)),
            jax.ShapeDtypeStruct((8, rows), f32), z_scratch, 25_000_000_000,
        )
        packet = jnp.concatenate([stats[:3], lab.astype(f32)[None, :]], axis=0)
        packets = lax.all_gather(packet, ("dp", "tp")).reshape(groups, shards, 4, rows)
        labs = packets[:, 0, 3, :].astype(i32)
        valid = labs >= 0
        maxes = jnp.where(valid[:, None, :], packets[:, :, 0, :], 0.0)
        row_max = jnp.max(maxes, axis=1)
        sum_exp = jnp.where(valid, jnp.sum(packets[:, :, 1, :] * jnp.exp(maxes - row_max[:, None, :]), axis=1), 1.0)
        target = jnp.sum(packets[:, :, 2, :], axis=1)
        lives = jnp.sum(valid, axis=1).astype(i32)
        denom = jnp.sum(lives).astype(f32) + LOSS_EPS
        loss = jnp.sum(jnp.where(valid, jnp.log(sum_exp) + row_max - target, 0.0)) / denom
        inv = 1.0 / denom
        metas = jnp.stack([
            jnp.where(valid, row_max, OFF),
            jnp.where(valid, (1.0 / sum_exp) * inv, 0.0),
            jnp.where(valid, inv, 0.0),
            jnp.where(valid, labs - me_tp * vocab, -1).astype(f32),
        ], axis=1)

        own_meta = lax.dynamic_index_in_dim(metas, me_dp, 0, keepdims=False)
        d_embed, d_bias_own, d_tok = run(
            own_kernel, (blocks,), VOCAB_BLOCKS, (local_lab[None, :], own_meta, tok, embed, bias),
            [whole((1, rows)), whole((4, rows)), whole((rows, width)), by_rows((height, width)), by_rows((height, 128))],
            [by_rows((height, width)), by_rows((height, 128)), whole((rows, width))],
            [jax.ShapeDtypeStruct((vocab, width), f32), jax.ShapeDtypeStruct((vocab, 128), f32), jax.ShapeDtypeStruct((rows, width), f32)],
            z_scratch + dz_scratch, 75_000_000_000,
        )
        d_normed = lax.psum(d_tok, "tp")

        cap = (groups - 1) * rows
        meta = jnp.concatenate([jnp.full((1, cap + TOK), OFF, f32), jnp.zeros((2, cap + TOK), f32), jnp.full((1, cap + TOK), -1.0, f32)], axis=0)
        pos = jnp.int32(0)
        ids = jnp.arange(cap // CHUNK, dtype=i32)
        src, dst, chunks = jnp.zeros_like(ids), jnp.zeros_like(ids), jnp.int32(0)
        for k in range(1, groups):
            peer = lax.rem(me_dp + k, groups)
            meta = lax.dynamic_update_slice(meta, lax.dynamic_index_in_dim(metas, peer, 0, keepdims=False), (0, pos))
            size = lax.dynamic_index_in_dim(lives, peer, 0, keepdims=False)
            parts = (size + CHUNK - 1) // CHUNK
            inside = ids >= chunks
            src = jnp.where(inside, peer * rows + (ids - chunks) * CHUNK, src)
            dst = jnp.where(inside, pos + (ids - chunks) * CHUNK, dst)
            chunks = chunks + parts
            last = pos + parts * CHUNK
            pos = pos + (size + 15) // 16 * 16
        plan = jnp.stack([(pos + TOK - 1) // TOK, chunks, last])
        meta_lab = meta[3:4].astype(i32)
        d_bias = d_bias_own
        for first, last_blk in ((0, SPLIT), (SPLIT, VOCAB_BLOCKS)):
            blk = functools.partial(by_rows, first=first)
            d_embed, d_bias = run(
                functools.partial(rest_kernel, first), (plan, src, dst), last_blk - first, (meta_lab, meta, embed, bias, d_embed, d_bias, tok_all),
                [whole((1, cap + TOK)), whole((4, cap + TOK)), blk((height, width)), blk((height, 128)), blk((height, width)), blk((height, 128)), pl.BlockSpec(memory_space=pl.ANY)],
                [blk((height, width)), blk((height, 128))],
                [jax.ShapeDtypeStruct((vocab, width), f32), jax.ShapeDtypeStruct((vocab, 128), f32)],
                [pltpu.VMEM((cap + TOK, width), bf16), pltpu.VMEM((STAGES, CHUNK, width), f32), pltpu.SemaphoreType.DMA((STAGES,))] + z_scratch + dz_scratch,
                25_000_000_000 * (last_blk - first), {7: 0, 8: 1},
            )
        d_out_bias = jnp.sum(d_bias, axis=1)

        d_pre, d_gamma, d_beta = norm_vjp(d_normed)
        d_pre_bf = d_pre.astype(bf16)
        d_w_t = jnp.einsum("nd,ne->de", picked, d_pre_bf, preferred_element_type=f32)
        d_b_t = jnp.sum(d_pre, axis=0)
        d_w_t = lax.psum(d_w_t, "dp")
        d_b_t, d_gamma, d_beta = lax.psum((d_b_t, d_gamma, d_beta), "dp")
        d_rows = jnp.einsum("ne,de->nd", d_pre_bf, w_t, preferred_element_type=f32)
        d_hidden = run(
            place_kernel, (base,), batch // SEQS, (idx_rows, d_rows),
            [by_rows((SEQS, 1, 128)), whole((rows, width))], by_rows((SEQS, seq_len, width)),
            jax.ShapeDtypeStruct((batch, seq_len, width), bf16), [], 8_000_000_000,
        )
        return loss, d_hidden, d_w_t, d_b_t, d_gamma, d_beta, d_embed, d_out_bias

    in_specs = (P("dp", None, None), P("dp", None), P("dp", None), P("dp", None), P(None, None), P(None), P(None), P(None), P("tp", None), P("tp"))
    out_specs = (P(), P("dp", None, None), P(None, None), P(None), P(None), P(None), P("tp", None), P("tp"))
    return jax.shard_map(local_step, mesh=mesh, in_specs=in_specs, out_specs=out_specs, check_vma=False)
```

```python
import functools

import jax
import jax.numpy as jnp
from jax import lax
from jax.experimental import pallas as pl
from jax.experimental.pallas import tpu as pltpu
from jax.sharding import PartitionSpec as P


LN_EPS = 1e-12
LOSS_EPS = 1e-5
VOCAB_BLOCKS = 6
TOK = 256
CHUNK = 256
STAGES = 4
PICK = 96
SEQS = 4
SPLIT = 4
OFF = 1e30
VMEM_LIMIT = 67_000_000


def gelu_norm(pre_act, gamma, beta):
    activated = jax.nn.gelu(pre_act, approximate=False)
    mean_val = jnp.mean(activated, axis=-1, keepdims=True)
    centered = activated - mean_val
    variance = jnp.mean(centered * centered, axis=-1, keepdims=True)
    return centered * lax.rsqrt(variance + LN_EPS) * gamma + beta


def dot_nt(a, b):
    return lax.dot_general(a, b, (((1,), (1,)), ((), ())), preferred_element_type=jnp.float32)


def dot_tn(a, b):
    return lax.dot_general(a, b, (((0,), (0,)), ((), ())), preferred_element_type=jnp.float32)


def dot_nn(a, b):
    return jnp.dot(a, b, preferred_element_type=jnp.float32)


def hot_rows(row, seq_len):
    ids = lax.broadcasted_iota(jnp.int32, (seq_len, PICK), 0)
    return jnp.where(ids == row[:, :PICK], 1.0, 0.0).astype(jnp.bfloat16)


def pick_kernel(base_ref, idx_ref, hidden_ref, out_ref, acc):
    step = pl.program_id(0)

    @pl.when(step == 0)
    def _():
        acc[...] = jnp.zeros_like(acc)

    picked = [dot_tn(hot_rows(idx_ref[k], hidden_ref.shape[1]), hidden_ref[k]) for k in range(SEQS)]
    for k, rows in enumerate(picked):
        base = pl.multiple_of(base_ref[step * SEQS + k], 8)
        acc[pl.ds(base, 16), :] += rows[:16]
        acc[pl.ds(base + 16, PICK - 16), :] = rows[16:]

    @pl.when(step == pl.num_programs(0) - 1)
    def _():
        out_ref[...] = acc[...].astype(jnp.bfloat16)


def place_kernel(base_ref, idx_ref, rows_ref, out_ref):
    step = pl.program_id(0)
    for k in range(SEQS):
        base = pl.multiple_of(base_ref[step * SEQS + k], 8)
        rows = rows_ref[pl.ds(base, PICK), :].astype(jnp.bfloat16)
        out_ref[k] = dot_nn(hot_rows(idx_ref[k], out_ref.shape[1]), rows).astype(jnp.bfloat16)


def for_blocks(count, body):
    def pair(step, carry):
        body(step, 2 * TOK)
        return carry

    lax.fori_loop(0, count // 2, pair, 0)

    @pl.when(count % 2 == 1)
    def _():
        body(count // 2, TOK)


def strips(height):
    size = (height // 4 + 15) // 16 * 16
    return [(at, min(size, height - at)) for at in range(0, height, size)]


def tile_bias(bias_ref, at, size, width):
    bias = bias_ref[at:at + size, :]
    return jnp.concatenate([bias] * (width // bias.shape[1]), axis=1)


def stats_kernel(count_ref, lab_ref, tok_ref, embed_ref, bias_ref, out_ref, logits_hbm, z_ref, sems):
    vblk = pl.program_id(0)
    height = embed_ref.shape[0]
    steps = (count_ref[0] + 1) // 2

    def save(vocab_blk, step, slot):
        return pltpu.make_async_copy(z_ref.at[slot], logits_hbm.at[vocab_blk, step], sems.at[slot])

    @pl.when(vblk == 0)
    def _():
        out_ref[...] = jnp.zeros_like(out_ref)
        out_ref[0:1, :] = jnp.full((1, out_ref.shape[1]), -jnp.inf, jnp.float32)

    def body(step, width):
        cols = pl.ds(pl.multiple_of(step * 2 * TOK, 2 * TOK), width)
        turn = vblk * steps + step
        slot = lax.rem(turn, 2)

        @pl.when(turn >= 2)
        def _():
            save(vblk, step, slot).wait()

        tok = tok_ref[cols, :]
        lab = lab_ref[0:1, cols] - vblk * height
        parts = []
        target = jnp.zeros((1, width), jnp.float32)
        for at, size in strips(height):
            z_ref[slot, at:at + size, :width] = dot_nt(embed_ref[at:at + size, :], tok) + tile_bias(bias_ref, at, size, width)
        for at, size in strips(height):
            z = z_ref[slot, at:at + size, :width]
            top = jnp.max(z, axis=0, keepdims=True)
            total = jnp.sum(jnp.exp(z - top), axis=0, keepdims=True)
            hit = lax.broadcasted_iota(jnp.int32, (size, width), 0) == lab - at
            target += jnp.sum(jnp.where(hit, z, 0.0), axis=0, keepdims=True)
            parts.append((top, total))
        old_max = out_ref[0:1, cols]
        new_max = functools.reduce(jnp.maximum, [top for top, _ in parts], old_max)
        total = out_ref[1:2, cols] * jnp.exp(old_max - new_max)
        for top, part in parts:
            total += part * jnp.exp(top - new_max)
        out_ref[0:1, cols] = new_max
        out_ref[1:2, cols] = total
        out_ref[2:3, cols] += target
        save(vblk, step, slot).start()

    for_blocks(count_ref[0], body)

    @pl.when(vblk == pl.num_programs(0) - 1)
    def _():
        turns = pl.num_programs(0) * steps
        save(0, 0, lax.rem(turns, 2)).wait()
        save(0, 0, lax.rem(turns + 1, 2)).wait()


def grad_strip(at, size, width, z, lab, top, scale, unit, dbias_ref, dz_ref, fresh=None):
    lanes = dbias_ref.shape[1]
    hit = lax.broadcasted_iota(jnp.int32, (size, width), 0) == lab - at
    dz = jnp.exp(z - top) * scale - jnp.where(hit, unit, 0.0)
    part = dz[:, :lanes]
    for j in range(1, width // lanes):
        part = part + dz[:, j * lanes:(j + 1) * lanes]
    old = dbias_ref[at:at + size, :]
    dbias_ref[at:at + size, :] = part + (old if fresh is None else jnp.where(fresh, 0.0, old))
    dz_ref[at:at + size, :width] = dz.astype(jnp.bfloat16)


def token_row(cols, vblk, height, lab_ref, meta_ref):
    return lab_ref[0:1, cols] - vblk * height, meta_ref[0:1, cols], meta_ref[1:2, cols], meta_ref[2:3, cols]


def own_kernel(count_ref, lab_ref, meta_ref, tok_ref, embed_ref, logits_hbm, dembed_ref, dbias_ref, dtok_ref, z_ref, sems, dz_ref):
    vblk = pl.program_id(0)
    height = embed_ref.shape[0]
    steps = (count_ref[0] + 1) // 2

    def load(vocab_blk, step, slot):
        return pltpu.make_async_copy(logits_hbm.at[vocab_blk, step], z_ref.at[slot], sems.at[slot])

    @pl.when(vblk == 0)
    def _():
        dtok_ref[...] = jnp.zeros_like(dtok_ref)
        load(0, 0, 0).start()

    def body(step, width):
        turn = vblk * steps + step
        slot = lax.rem(turn, 2)
        wrap = step + 1 == steps
        next_blk, next_step = jnp.where(wrap, vblk + 1, vblk), jnp.where(wrap, 0, step + 1)

        @pl.when(next_blk < pl.num_programs(0))
        def _():
            load(next_blk, next_step, 1 - slot).start()

        load(vblk, step, slot).wait()
        cols = pl.ds(pl.multiple_of(step * 2 * TOK, 2 * TOK), width)
        tok = tok_ref[cols, :]
        row = token_row(cols, vblk, height, lab_ref, meta_ref)
        fresh = step == 0
        todo = strips(height)

        def grad(at, size):
            grad_strip(at, size, width, z_ref[slot, at:at + size, :width], *row, dbias_ref, dz_ref, fresh)

        grad(*todo[0])
        for k, (at, size) in enumerate(todo):
            if k + 1 < len(todo):
                grad(*todo[k + 1])
            dz = dz_ref[at:at + size, :width]
            dembed_ref[at:at + size, :] = dot_nn(dz, tok) + jnp.where(fresh, 0.0, dembed_ref[at:at + size, :])
        dtok_ref[cols, :] += dot_tn(dz_ref[:, :width], embed_ref[...])

    for_blocks(count_ref[0], body)


def rest_kernel(first, plan_ref, src_ref, dst_ref, lab_ref, meta_ref, embed_ref, bias_ref, dembed_in_ref, dbias_in_ref, tok_hbm, dembed_ref, dbias_ref, tok_ref, stage, sems, z_ref, dz_ref):
    vblk = pl.program_id(0)
    chunks = plan_ref[1]

    def fetch(chunk):
        slot = lax.rem(chunk, STAGES)
        src = tok_hbm.at[pl.ds(pl.multiple_of(src_ref[chunk], CHUNK), CHUNK), :]
        return pltpu.make_async_copy(src, stage.at[slot], sems.at[slot])

    @pl.when(vblk == 0)
    def _():
        end = pl.multiple_of(plan_ref[2], 16)
        tok_ref[pl.ds(end, TOK), :] = jnp.zeros((TOK, tok_ref.shape[1]), jnp.bfloat16)
        for k in range(STAGES):
            @pl.when(k < chunks)
            def _():
                fetch(k).start()

        def take(chunk, carry):
            fetch(chunk).wait()
            dst = pl.multiple_of(dst_ref[chunk], 16)
            tok_ref[pl.ds(dst, CHUNK), :] = stage[lax.rem(chunk, STAGES)].astype(jnp.bfloat16)

            @pl.when(chunk + STAGES < chunks)
            def _():
                fetch(chunk + STAGES).start()

            return carry

        lax.fori_loop(0, chunks, take, 0)

    dembed_ref[...] = dembed_in_ref[...]
    dbias_ref[...] = dbias_in_ref[...]

    height = embed_ref.shape[0]

    def body(step, width):
        cols = pl.ds(pl.multiple_of(step * 2 * TOK, 2 * TOK), width)
        tok = tok_ref[cols, :]
        row = token_row(cols, vblk + first, height, lab_ref, meta_ref)
        todo = strips(height)

        def logits(at, size):
            z_ref[at:at + size, :width] = dot_nt(embed_ref[at:at + size, :], tok)

        logits(*todo[0])
        for k, (at, size) in enumerate(todo):
            if k + 1 < len(todo):
                logits(*todo[k + 1])
            grad_strip(at, size, width, z_ref[at:at + size, :width] + tile_bias(bias_ref, at, size, width), *row, dbias_ref, dz_ref)
            dembed_ref[at:at + size, :] += dot_nn(dz_ref[at:at + size, :width], tok)

    for_blocks(plan_ref[0], body)


def whole(shape):
    return pl.BlockSpec(shape, lambda *_: (0,) * len(shape))


def by_rows(shape, first=0):
    return pl.BlockSpec(shape, lambda step, *_: (step + first,) + (0,) * (len(shape) - 1))


def run(kernel, scalars, grid, args, in_specs, out_specs, out_shape, scratch, flops, aliases=None):
    return pl.pallas_call(
        kernel,
        grid_spec=pltpu.PrefetchScalarGridSpec(
            num_scalar_prefetch=len(scalars), grid=(grid,), in_specs=in_specs, out_specs=out_specs, scratch_shapes=scratch
        ),
        out_shape=out_shape,
        input_output_aliases=aliases or {},
        compiler_params=pltpu.CompilerParams(dimension_semantics=("arbitrary",), vmem_limit_bytes=VMEM_LIMIT),
        cost_estimate=pl.CostEstimate(flops=flops, bytes_accessed=40_000_000, transcendentals=0),
    )(*scalars, *args)


def solution(mesh):
    groups, shards = mesh.shape["dp"], mesh.shape["tp"]
    f32, bf16, i32 = jnp.float32, jnp.bfloat16, jnp.int32

    def local_step(hidden, positions, labels, weights, w_t, b_t, gamma, beta, embed, out_bias):
        batch, seq_len, width = hidden.shape
        max_pred = positions.shape[1]
        rows = batch * max_pred
        vocab = embed.shape[0]
        height = vocab // VOCAB_BLOCKS
        me_dp, me_tp = lax.axis_index("dp"), lax.axis_index("tp")

        live = jnp.sum(weights, axis=1).astype(i32)
        seqs = jnp.arange(batch, dtype=i32)
        offset = jnp.sum(jnp.where(seqs[None, :] < seqs[:, None], live[None, :], 0), axis=1)
        base = jnp.minimum(offset // 8 * 8, rows - PICK)
        slots = jnp.arange(max_pred, dtype=i32)
        alive = slots[None, :] < live[:, None]
        place = jnp.where(alive, slots[None, :] + (offset - base)[:, None], -1)
        lanes = jnp.arange(128, dtype=i32)
        idx_rows = jnp.sum(jnp.where(place[:, None, :] == lanes[None, :, None], positions[:, None, :] + 1, 0), axis=2) - 1
        idx_rows = idx_rows.reshape(batch, 1, 128)
        packed = jnp.where(alive, slots[None, :] + offset[:, None], -1).reshape(-1)
        lab = jnp.sum(jnp.where(packed[None, :] == jnp.arange(rows, dtype=i32)[:, None], labels.reshape(-1)[None, :] + 1, 0), axis=1) - 1
        count = jnp.sum(live)
        blocks = ((count + TOK - 1) // TOK).reshape(1)

        picked = run(
            pick_kernel, (base,), batch // SEQS, (idx_rows, hidden),
            [by_rows((SEQS, 1, 128)), by_rows((SEQS, seq_len, width))], whole((rows, width)),
            jax.ShapeDtypeStruct((rows, width), bf16), [pltpu.VMEM((rows, width), f32)], 8_000_000_000,
        )
        pre_act = jnp.dot(picked, w_t, preferred_element_type=f32) + b_t
        normed, norm_vjp = jax.vjp(gelu_norm, pre_act, gamma, beta)
        tok = normed.astype(bf16)
        share = rows // shards
        mine = lax.dynamic_slice(normed, (me_tp * share, 0), (share, width))
        tok_all = lax.all_gather(mine, ("dp", "tp"), tiled=True)

        bias = jnp.broadcast_to(out_bias[:, None], (vocab, 128))
        local_lab = jnp.where(lab >= 0, lab - me_tp * vocab, -1)
        z_scratch = [pltpu.VMEM((height, 2 * TOK), f32)]
        dz_scratch = [pltpu.VMEM((height, 2 * TOK), bf16)]
        logit_shape = (VOCAB_BLOCKS, -(-rows // (2 * TOK)), height, 2 * TOK)
        slots_scratch = [pltpu.VMEM((2, height, 2 * TOK), f32), pltpu.SemaphoreType.DMA((2,))]
        anywhere = pl.BlockSpec(memory_space=pl.ANY)
        stats, logits = run(
            stats_kernel, (blocks,), VOCAB_BLOCKS, (local_lab[None, :], tok, embed, bias),
            [whole((1, rows)), whole((rows, width)), by_rows((height, width)), by_rows((height, 128))], [whole((8, rows)), anywhere],
            [jax.ShapeDtypeStruct((8, rows), f32), jax.ShapeDtypeStruct(logit_shape, f32)], slots_scratch, 25_000_000_000,
        )
        packet = jnp.concatenate([stats[:3], lab.astype(f32)[None, :]], axis=0)
        packets = lax.all_gather(packet, ("dp", "tp")).reshape(groups, shards, 4, rows)
        labs = packets[:, 0, 3, :].astype(i32)
        valid = labs >= 0
        maxes = jnp.where(valid[:, None, :], packets[:, :, 0, :], 0.0)
        row_max = jnp.max(maxes, axis=1)
        sum_exp = jnp.where(valid, jnp.sum(packets[:, :, 1, :] * jnp.exp(maxes - row_max[:, None, :]), axis=1), 1.0)
        target = jnp.sum(packets[:, :, 2, :], axis=1)
        lives = jnp.sum(valid, axis=1).astype(i32)
        denom = jnp.sum(lives).astype(f32) + LOSS_EPS
        loss = jnp.sum(jnp.where(valid, jnp.log(sum_exp) + row_max - target, 0.0)) / denom
        inv = 1.0 / denom
        metas = jnp.stack([
            jnp.where(valid, row_max, OFF),
            jnp.where(valid, (1.0 / sum_exp) * inv, 0.0),
            jnp.where(valid, inv, 0.0),
            jnp.where(valid, labs - me_tp * vocab, -1).astype(f32),
        ], axis=1)

        own_meta = lax.dynamic_index_in_dim(metas, me_dp, 0, keepdims=False)
        d_embed, d_bias_own, d_tok = run(
            own_kernel, (blocks,), VOCAB_BLOCKS, (local_lab[None, :], own_meta, tok, embed, logits),
            [whole((1, rows)), whole((4, rows)), whole((rows, width)), by_rows((height, width)), anywhere],
            [by_rows((height, width)), by_rows((height, 128)), whole((rows, width))],
            [jax.ShapeDtypeStruct((vocab, width), f32), jax.ShapeDtypeStruct((vocab, 128), f32), jax.ShapeDtypeStruct((rows, width), f32)],
            slots_scratch + dz_scratch, 50_000_000_000,
        )
        d_normed = lax.psum(d_tok, "tp")

        cap = (groups - 1) * rows
        meta = jnp.concatenate([jnp.full((1, cap + TOK), OFF, f32), jnp.zeros((2, cap + TOK), f32), jnp.full((1, cap + TOK), -1.0, f32)], axis=0)
        pos = jnp.int32(0)
        ids = jnp.arange(cap // CHUNK, dtype=i32)
        src, dst, chunks = jnp.zeros_like(ids), jnp.zeros_like(ids), jnp.int32(0)
        for k in range(1, groups):
            peer = lax.rem(me_dp + k, groups)
            meta = lax.dynamic_update_slice(meta, lax.dynamic_index_in_dim(metas, peer, 0, keepdims=False), (0, pos))
            size = lax.dynamic_index_in_dim(lives, peer, 0, keepdims=False)
            parts = (size + CHUNK - 1) // CHUNK
            inside = ids >= chunks
            src = jnp.where(inside, peer * rows + (ids - chunks) * CHUNK, src)
            dst = jnp.where(inside, pos + (ids - chunks) * CHUNK, dst)
            chunks = chunks + parts
            last = pos + parts * CHUNK
            pos = pos + (size + 15) // 16 * 16
        plan = jnp.stack([(pos + TOK - 1) // TOK, chunks, last])
        meta_lab = meta[3:4].astype(i32)
        d_bias = d_bias_own
        for first, last_blk in ((0, SPLIT), (SPLIT, VOCAB_BLOCKS)):
            blk = functools.partial(by_rows, first=first)
            d_embed, d_bias = run(
                functools.partial(rest_kernel, first), (plan, src, dst), last_blk - first, (meta_lab, meta, embed, bias, d_embed, d_bias, tok_all),
                [whole((1, cap + TOK)), whole((4, cap + TOK)), blk((height, width)), blk((height, 128)), blk((height, width)), blk((height, 128)), pl.BlockSpec(memory_space=pl.ANY)],
                [blk((height, width)), blk((height, 128))],
                [jax.ShapeDtypeStruct((vocab, width), f32), jax.ShapeDtypeStruct((vocab, 128), f32)],
                [pltpu.VMEM((cap + TOK, width), bf16), pltpu.VMEM((STAGES, CHUNK, width), f32), pltpu.SemaphoreType.DMA((STAGES,))] + z_scratch + dz_scratch,
                25_000_000_000 * (last_blk - first), {7: 0, 8: 1},
            )
        d_out_bias = jnp.sum(d_bias, axis=1)

        d_pre, d_gamma, d_beta = norm_vjp(d_normed)
        d_pre_bf = d_pre.astype(bf16)
        d_w_t = jnp.einsum("nd,ne->de", picked, d_pre_bf, preferred_element_type=f32)
        d_b_t = jnp.sum(d_pre, axis=0)
        small = jnp.stack([d_b_t, d_gamma, d_beta] + [jnp.zeros_like(d_b_t)] * 5)
        sums = lax.psum(jnp.concatenate([d_w_t, small], axis=0), "dp")
        d_w_t, d_b_t, d_gamma, d_beta = sums[:width], sums[width], sums[width + 1], sums[width + 2]
        d_rows = jnp.einsum("ne,de->nd", d_pre_bf, w_t, preferred_element_type=f32)
        d_hidden = run(
            place_kernel, (base,), batch // SEQS, (idx_rows, d_rows),
            [by_rows((SEQS, 1, 128)), whole((rows, width))], by_rows((SEQS, seq_len, width)),
            jax.ShapeDtypeStruct((batch, seq_len, width), bf16), [], 8_000_000_000,
        )
        return loss, d_hidden, d_w_t, d_b_t, d_gamma, d_beta, d_embed, d_out_bias

    in_specs = (P("dp", None, None), P("dp", None), P("dp", None), P("dp", None), P(None, None), P(None), P(None), P(None), P("tp", None), P("tp"))
    out_specs = (P(), P("dp", None, None), P(None, None), P(None), P(None), P(None), P("tp", None), P("tp"))
    return jax.shard_map(local_step, mesh=mesh, in_specs=in_specs, out_specs=out_specs, check_vma=False)
```

```python
import functools
import math

import jax
import jax.numpy as jnp
from jax import lax
from jax.experimental import pallas as pl
from jax.experimental.pallas import tpu as pltpu
from jax.sharding import PartitionSpec as P


LN_EPS = 1e-12
LOSS_EPS = 1e-5
SQRT_HALF = 0.5 ** 0.5
BELL_PEAK = (2.0 * math.pi) ** -0.5
VOCAB_BLOCKS = 6
TOK = 256
CHUNK = 256
STAGES = 4
PICK = 96
SEQS = 4
SPLIT = 4
OFF = 1e30
VMEM_LIMIT = 67_000_000


def normalize(pre_act):
    bell = 0.5 * (1.0 + lax.erf(pre_act * SQRT_HALF))
    activated = pre_act * bell
    centered = activated - jnp.mean(activated, axis=-1, keepdims=True)
    scale = lax.rsqrt(jnp.mean(centered * centered, axis=-1, keepdims=True) + LN_EPS)
    return centered * scale, scale, bell


def dot_nt(a, b):
    return lax.dot_general(a, b, (((1,), (1,)), ((), ())), preferred_element_type=jnp.float32)


def dot_tn(a, b):
    return lax.dot_general(a, b, (((0,), (0,)), ((), ())), preferred_element_type=jnp.float32)


def dot_nn(a, b):
    return jnp.dot(a, b, preferred_element_type=jnp.float32)


def hot_rows(row, seq_len):
    ids = lax.broadcasted_iota(jnp.int32, (seq_len, PICK), 0)
    return jnp.where(ids == row[:, :PICK], 1.0, 0.0).astype(jnp.bfloat16)


def pick_kernel(base_ref, count_ref, idx_ref, hidden_ref, weight_ref, vecs_ref, picked_ref, normed_ref, tok_ref, acc):
    step = pl.program_id(0)
    picks = base_ref.shape[0] // SEQS
    block = step - picks

    @pl.when(step == 0)
    def _():
        acc[...] = jnp.zeros_like(acc)

    @pl.when(step < picks)
    def _():
        picked = [dot_tn(hot_rows(idx_ref[k], hidden_ref.shape[1]), hidden_ref[k]) for k in range(SEQS)]
        for k, rows in enumerate(picked):
            base = pl.multiple_of(base_ref[step * SEQS + k], 8)
            acc[pl.ds(base, 16), :] += rows[:16]
            acc[pl.ds(base + 16, PICK - 16), :] = rows[16:]

    @pl.when(step >= picks)
    def _():
        rows = acc[pl.ds(pl.multiple_of(block * TOK, TOK), TOK), :].astype(jnp.bfloat16)
        picked_ref[...] = rows

        @pl.when(block * TOK < count_ref[0])
        def _():
            unit, _, _ = normalize(dot_nn(rows, weight_ref[...]) + vecs_ref[0:1, :])
            normed = unit * vecs_ref[1:2, :] + vecs_ref[2:3, :]
            normed_ref[...] = normed
            tok_ref[...] = normed.astype(jnp.bfloat16)

        @pl.when(block * TOK >= count_ref[0])
        def _():
            normed_ref[...] = jnp.zeros_like(normed_ref)
            tok_ref[...] = jnp.zeros_like(tok_ref)


def back_kernel(base_ref, count_ref, idx_ref, dnormed_ref, picked_ref, weight_ref, vecs_ref, sums_ref, dhidden_ref, drows):
    step = pl.program_id(0)
    blocks = drows.shape[0] // TOK
    width = weight_ref.shape[0]

    @pl.when(step == 0)
    def _():
        sums_ref[...] = jnp.zeros_like(sums_ref)
        drows[...] = jnp.zeros_like(drows)

    @pl.when((step < blocks) & (step * TOK < count_ref[0]))
    def _():
        pre_act = dot_nn(picked_ref[...], weight_ref[...]) + vecs_ref[0:1, :]
        unit, scale, bell = normalize(pre_act)
        dnormed = dnormed_ref[...]
        dunit = dnormed * vecs_ref[1:2, :]
        dcentered = scale * (dunit - unit * jnp.mean(dunit * unit, axis=-1, keepdims=True))
        dactivated = dcentered - jnp.mean(dcentered, axis=-1, keepdims=True)
        slope = bell + pre_act * (BELL_PEAK * jnp.exp(-0.5 * pre_act * pre_act))
        dpre = dactivated * slope
        dpre_bf = dpre.astype(jnp.bfloat16)
        sums_ref[:width, :] += dot_tn(picked_ref[...], dpre_bf)
        sums_ref[width:width + 1, :] += jnp.sum(dpre, axis=0, keepdims=True)
        sums_ref[width + 1:width + 2, :] += jnp.sum(dnormed * unit, axis=0, keepdims=True)
        sums_ref[width + 2:width + 3, :] += jnp.sum(dnormed, axis=0, keepdims=True)
        drows[pl.ds(pl.multiple_of(step * TOK, TOK), TOK), :] = dot_nt(dpre_bf, weight_ref[...])

    @pl.when(step >= blocks)
    def _():
        for k in range(SEQS):
            base = pl.multiple_of(base_ref[(step - blocks) * SEQS + k], 8)
            rows = drows[pl.ds(base, PICK), :].astype(jnp.bfloat16)
            dhidden_ref[k] = dot_nn(hot_rows(idx_ref[k], dhidden_ref.shape[1]), rows).astype(jnp.bfloat16)


def for_blocks(count, body):
    def pair(step, carry):
        body(step, 2 * TOK)
        return carry

    lax.fori_loop(0, count // 2, pair, 0)

    @pl.when(count % 2 == 1)
    def _():
        body(count // 2, TOK)


def strips(height):
    size = (height // 4 + 15) // 16 * 16
    return [(at, min(size, height - at)) for at in range(0, height, size)]


def tile_bias(bias_ref, at, size, width):
    bias = bias_ref[at:at + size, :]
    return jnp.concatenate([bias] * (width // bias.shape[1]), axis=1)


def stats_kernel(count_ref, lab_ref, tok_ref, embed_ref, bias_ref, out_ref, logits_hbm, z_ref, sems):
    vblk = pl.program_id(0)
    height = embed_ref.shape[0]
    steps = (count_ref[0] + 1) // 2

    def save(vocab_blk, step, slot):
        return pltpu.make_async_copy(z_ref.at[slot], logits_hbm.at[vocab_blk, step], sems.at[slot])

    @pl.when(vblk == 0)
    def _():
        out_ref[...] = jnp.zeros_like(out_ref)
        out_ref[0:1, :] = jnp.full((1, out_ref.shape[1]), -jnp.inf, jnp.float32)

    def body(step, width):
        cols = pl.ds(pl.multiple_of(step * 2 * TOK, 2 * TOK), width)
        turn = vblk * steps + step
        slot = lax.rem(turn, 2)

        @pl.when(turn >= 2)
        def _():
            save(vblk, step, slot).wait()

        tok = tok_ref[cols, :]
        lab = lab_ref[0:1, cols] - vblk * height
        parts = []
        target = jnp.zeros((1, width), jnp.float32)
        for at, size in strips(height):
            z_ref[slot, at:at + size, :width] = dot_nt(embed_ref[at:at + size, :], tok) + tile_bias(bias_ref, at, size, width)
        for at, size in strips(height):
            z = z_ref[slot, at:at + size, :width]
            top = jnp.max(z, axis=0, keepdims=True)
            total = jnp.sum(jnp.exp(z - top), axis=0, keepdims=True)
            hit = lax.broadcasted_iota(jnp.int32, (size, width), 0) == lab - at
            target += jnp.sum(jnp.where(hit, z, 0.0), axis=0, keepdims=True)
            parts.append((top, total))
        old_max = out_ref[0:1, cols]
        new_max = functools.reduce(jnp.maximum, [top for top, _ in parts], old_max)
        total = out_ref[1:2, cols] * jnp.exp(old_max - new_max)
        for top, part in parts:
            total += part * jnp.exp(top - new_max)
        out_ref[0:1, cols] = new_max
        out_ref[1:2, cols] = total
        out_ref[2:3, cols] += target
        save(vblk, step, slot).start()

    for_blocks(count_ref[0], body)

    @pl.when(vblk == pl.num_programs(0) - 1)
    def _():
        turns = pl.num_programs(0) * steps
        save(0, 0, lax.rem(turns, 2)).wait()
        save(0, 0, lax.rem(turns + 1, 2)).wait()


def grad_strip(at, size, width, z, lab, top, scale, unit, dbias_ref, dz_ref, fresh=None):
    lanes = dbias_ref.shape[1]
    hit = lax.broadcasted_iota(jnp.int32, (size, width), 0) == lab - at
    dz = jnp.exp(z - top) * scale - jnp.where(hit, unit, 0.0)
    part = dz[:, :lanes]
    for j in range(1, width // lanes):
        part = part + dz[:, j * lanes:(j + 1) * lanes]
    old = dbias_ref[at:at + size, :]
    dbias_ref[at:at + size, :] = part + (old if fresh is None else jnp.where(fresh, 0.0, old))
    dz_ref[at:at + size, :width] = dz.astype(jnp.bfloat16)


def token_row(cols, vblk, height, lab_ref, meta_ref):
    return lab_ref[0:1, cols] - vblk * height, meta_ref[0:1, cols], meta_ref[1:2, cols], meta_ref[2:3, cols]


def own_kernel(count_ref, lab_ref, meta_ref, tok_ref, embed_ref, logits_hbm, dembed_ref, dbias_ref, dtok_ref, z_ref, sems, dz_ref):
    vblk = pl.program_id(0)
    height = embed_ref.shape[0]
    steps = (count_ref[0] + 1) // 2

    def load(vocab_blk, step, slot):
        return pltpu.make_async_copy(logits_hbm.at[vocab_blk, step], z_ref.at[slot], sems.at[slot])

    @pl.when(vblk == 0)
    def _():
        dtok_ref[...] = jnp.zeros_like(dtok_ref)
        load(0, 0, 0).start()

    def body(step, width):
        turn = vblk * steps + step
        slot = lax.rem(turn, 2)
        wrap = step + 1 == steps
        next_blk, next_step = jnp.where(wrap, vblk + 1, vblk), jnp.where(wrap, 0, step + 1)

        @pl.when(next_blk < pl.num_programs(0))
        def _():
            load(next_blk, next_step, 1 - slot).start()

        load(vblk, step, slot).wait()
        cols = pl.ds(pl.multiple_of(step * 2 * TOK, 2 * TOK), width)
        tok = tok_ref[cols, :]
        row = token_row(cols, vblk, height, lab_ref, meta_ref)
        fresh = step == 0
        todo = strips(height)

        def grad(at, size):
            grad_strip(at, size, width, z_ref[slot, at:at + size, :width], *row, dbias_ref, dz_ref, fresh)

        grad(*todo[0])
        for k, (at, size) in enumerate(todo):
            if k + 1 < len(todo):
                grad(*todo[k + 1])
            dz = dz_ref[at:at + size, :width]
            dembed_ref[at:at + size, :] = dot_nn(dz, tok) + jnp.where(fresh, 0.0, dembed_ref[at:at + size, :])
        dtok_ref[cols, :] += dot_tn(dz_ref[:, :width], embed_ref[...])

    for_blocks(count_ref[0], body)


def rest_kernel(first, plan_ref, src_ref, dst_ref, lab_ref, meta_ref, embed_ref, bias_ref, dembed_in_ref, dbias_in_ref, tok_hbm, dembed_ref, dbias_ref, tok_ref, stage, sems, z_ref, dz_ref):
    vblk = pl.program_id(0)
    chunks = plan_ref[1]

    def fetch(chunk):
        slot = lax.rem(chunk, STAGES)
        src = tok_hbm.at[pl.ds(pl.multiple_of(src_ref[chunk], CHUNK), CHUNK), :]
        return pltpu.make_async_copy(src, stage.at[slot], sems.at[slot])

    @pl.when(vblk == 0)
    def _():
        end = pl.multiple_of(plan_ref[2], 16)
        tok_ref[pl.ds(end, TOK), :] = jnp.zeros((TOK, tok_ref.shape[1]), jnp.bfloat16)
        for k in range(STAGES):
            @pl.when(k < chunks)
            def _():
                fetch(k).start()

        def take(chunk, carry):
            fetch(chunk).wait()
            dst = pl.multiple_of(dst_ref[chunk], 16)
            tok_ref[pl.ds(dst, CHUNK), :] = stage[lax.rem(chunk, STAGES)].astype(jnp.bfloat16)

            @pl.when(chunk + STAGES < chunks)
            def _():
                fetch(chunk + STAGES).start()

            return carry

        lax.fori_loop(0, chunks, take, 0)

    dembed_ref[...] = dembed_in_ref[...]
    dbias_ref[...] = dbias_in_ref[...]

    height = embed_ref.shape[0]

    def body(step, width):
        cols = pl.ds(pl.multiple_of(step * 2 * TOK, 2 * TOK), width)
        tok = tok_ref[cols, :]
        row = token_row(cols, vblk + first, height, lab_ref, meta_ref)
        todo = strips(height)

        def logits(at, size):
            z_ref[at:at + size, :width] = dot_nt(embed_ref[at:at + size, :], tok)

        logits(*todo[0])
        for k, (at, size) in enumerate(todo):
            if k + 1 < len(todo):
                logits(*todo[k + 1])
            grad_strip(at, size, width, z_ref[at:at + size, :width] + tile_bias(bias_ref, at, size, width), *row, dbias_ref, dz_ref)
            dembed_ref[at:at + size, :] += dot_nn(dz_ref[at:at + size, :width], tok)

    for_blocks(plan_ref[0], body)


def whole(shape):
    return pl.BlockSpec(shape, lambda *_: (0,) * len(shape))


def by_rows(shape, first=0):
    return pl.BlockSpec(shape, lambda step, *_: (step + first,) + (0,) * (len(shape) - 1))


def run(kernel, scalars, grid, args, in_specs, out_specs, out_shape, scratch, flops, aliases=None):
    return pl.pallas_call(
        kernel,
        grid_spec=pltpu.PrefetchScalarGridSpec(
            num_scalar_prefetch=len(scalars), grid=(grid,), in_specs=in_specs, out_specs=out_specs, scratch_shapes=scratch
        ),
        out_shape=out_shape,
        input_output_aliases=aliases or {},
        compiler_params=pltpu.CompilerParams(dimension_semantics=("arbitrary",), vmem_limit_bytes=VMEM_LIMIT),
        cost_estimate=pl.CostEstimate(flops=flops, bytes_accessed=40_000_000, transcendentals=0),
    )(*scalars, *args)


def solution(mesh):
    groups, shards = mesh.shape["dp"], mesh.shape["tp"]
    f32, bf16, i32 = jnp.float32, jnp.bfloat16, jnp.int32

    def local_step(hidden, positions, labels, weights, w_t, b_t, gamma, beta, embed, out_bias):
        batch, seq_len, width = hidden.shape
        max_pred = positions.shape[1]
        rows = batch * max_pred
        vocab = embed.shape[0]
        height = vocab // VOCAB_BLOCKS
        me_dp, me_tp = lax.axis_index("dp"), lax.axis_index("tp")

        live = jnp.sum(weights, axis=1).astype(i32)
        seqs = jnp.arange(batch, dtype=i32)
        offset = jnp.sum(jnp.where(seqs[None, :] < seqs[:, None], live[None, :], 0), axis=1)
        base = jnp.minimum(offset // 8 * 8, rows - PICK)
        slots = jnp.arange(max_pred, dtype=i32)
        alive = slots[None, :] < live[:, None]
        place = jnp.where(alive, slots[None, :] + (offset - base)[:, None], -1)
        lanes = jnp.arange(128, dtype=i32)
        idx_rows = jnp.sum(jnp.where(place[:, None, :] == lanes[None, :, None], positions[:, None, :] + 1, 0), axis=2) - 1
        idx_rows = idx_rows.reshape(batch, 1, 128)
        packed = jnp.where(alive, slots[None, :] + offset[:, None], -1).reshape(-1)
        lab = jnp.sum(jnp.where(packed[None, :] == jnp.arange(rows, dtype=i32)[:, None], labels.reshape(-1)[None, :] + 1, 0), axis=1) - 1
        count = jnp.sum(live)
        blocks = ((count + TOK - 1) // TOK).reshape(1)

        picks, row_blocks = batch // SEQS, rows // TOK
        vecs = jnp.stack([b_t, gamma, beta] + [jnp.zeros_like(b_t)] * 5)
        early = lambda shape: pl.BlockSpec(shape, lambda step, *_: (jnp.minimum(step, picks - 1),) + (0,) * (len(shape) - 1))
        late = pl.BlockSpec((TOK, width), lambda step, *_: (jnp.maximum(step - picks, 0), 0))
        picked, normed, tok = run(
            pick_kernel, (base, count.reshape(1)), picks + row_blocks, (idx_rows, hidden, w_t, vecs),
            [early((SEQS, 1, 128)), early((SEQS, seq_len, width)), whole((width, width)), whole((8, width))], [late] * 3,
            [jax.ShapeDtypeStruct((rows, width), bf16), jax.ShapeDtypeStruct((rows, width), f32), jax.ShapeDtypeStruct((rows, width), bf16)],
            [pltpu.VMEM((rows, width), f32)], 8_000_000_000,
        )
        share = rows // shards
        mine = lax.dynamic_slice(normed, (me_tp * share, 0), (share, width))
        tok_all = lax.all_gather(mine, ("dp", "tp"), tiled=True)

        bias = jnp.broadcast_to(out_bias[:, None], (vocab, 128))
        local_lab = jnp.where(lab >= 0, lab - me_tp * vocab, -1)
        z_scratch = [pltpu.VMEM((height, 2 * TOK), f32)]
        dz_scratch = [pltpu.VMEM((height, 2 * TOK), bf16)]
        logit_shape = (VOCAB_BLOCKS, -(-rows // (2 * TOK)), height, 2 * TOK)
        slots_scratch = [pltpu.VMEM((2, height, 2 * TOK), f32), pltpu.SemaphoreType.DMA((2,))]
        anywhere = pl.BlockSpec(memory_space=pl.ANY)
        stats, logits = run(
            stats_kernel, (blocks,), VOCAB_BLOCKS, (local_lab[None, :], tok, embed, bias),
            [whole((1, rows)), whole((rows, width)), by_rows((height, width)), by_rows((height, 128))], [whole((8, rows)), anywhere],
            [jax.ShapeDtypeStruct((8, rows), f32), jax.ShapeDtypeStruct(logit_shape, f32)], slots_scratch, 25_000_000_000,
        )
        packet = jnp.concatenate([stats[:3], lab.astype(f32)[None, :]], axis=0)
        packets = lax.all_gather(packet, ("dp", "tp")).reshape(groups, shards, 4, rows)
        labs = packets[:, 0, 3, :].astype(i32)
        valid = labs >= 0
        maxes = jnp.where(valid[:, None, :], packets[:, :, 0, :], 0.0)
        row_max = jnp.max(maxes, axis=1)
        sum_exp = jnp.where(valid, jnp.sum(packets[:, :, 1, :] * jnp.exp(maxes - row_max[:, None, :]), axis=1), 1.0)
        target = jnp.sum(packets[:, :, 2, :], axis=1)
        lives = jnp.sum(valid, axis=1).astype(i32)
        denom = jnp.sum(lives).astype(f32) + LOSS_EPS
        loss = jnp.sum(jnp.where(valid, jnp.log(sum_exp) + row_max - target, 0.0)) / denom
        inv = 1.0 / denom
        metas = jnp.stack([
            jnp.where(valid, row_max, OFF),
            jnp.where(valid, (1.0 / sum_exp) * inv, 0.0),
            jnp.where(valid, inv, 0.0),
            jnp.where(valid, labs - me_tp * vocab, -1).astype(f32),
        ], axis=1)

        own_meta = lax.dynamic_index_in_dim(metas, me_dp, 0, keepdims=False)
        d_embed, d_bias_own, d_tok = run(
            own_kernel, (blocks,), VOCAB_BLOCKS, (local_lab[None, :], own_meta, tok, embed, logits),
            [whole((1, rows)), whole((4, rows)), whole((rows, width)), by_rows((height, width)), anywhere],
            [by_rows((height, width)), by_rows((height, 128)), whole((rows, width))],
            [jax.ShapeDtypeStruct((vocab, width), f32), jax.ShapeDtypeStruct((vocab, 128), f32), jax.ShapeDtypeStruct((rows, width), f32)],
            slots_scratch + dz_scratch, 50_000_000_000,
        )
        d_normed = lax.psum(d_tok, "tp")

        cap = (groups - 1) * rows
        meta = jnp.concatenate([jnp.full((1, cap + TOK), OFF, f32), jnp.zeros((2, cap + TOK), f32), jnp.full((1, cap + TOK), -1.0, f32)], axis=0)
        pos = jnp.int32(0)
        ids = jnp.arange(cap // CHUNK, dtype=i32)
        src, dst, chunks = jnp.zeros_like(ids), jnp.zeros_like(ids), jnp.int32(0)
        for k in range(1, groups):
            peer = lax.rem(me_dp + k, groups)
            meta = lax.dynamic_update_slice(meta, lax.dynamic_index_in_dim(metas, peer, 0, keepdims=False), (0, pos))
            size = lax.dynamic_index_in_dim(lives, peer, 0, keepdims=False)
            parts = (size + CHUNK - 1) // CHUNK
            inside = ids >= chunks
            src = jnp.where(inside, peer * rows + (ids - chunks) * CHUNK, src)
            dst = jnp.where(inside, pos + (ids - chunks) * CHUNK, dst)
            chunks = chunks + parts
            last = pos + parts * CHUNK
            pos = pos + (size + 15) // 16 * 16
        plan = jnp.stack([(pos + TOK - 1) // TOK, chunks, last])
        meta_lab = meta[3:4].astype(i32)
        d_bias = d_bias_own
        for first, last_blk in ((0, SPLIT), (SPLIT, VOCAB_BLOCKS)):
            blk = functools.partial(by_rows, first=first)
            d_embed, d_bias = run(
                functools.partial(rest_kernel, first), (plan, src, dst), last_blk - first, (meta_lab, meta, embed, bias, d_embed, d_bias, tok_all),
                [whole((1, cap + TOK)), whole((4, cap + TOK)), blk((height, width)), blk((height, 128)), blk((height, width)), blk((height, 128)), pl.BlockSpec(memory_space=pl.ANY)],
                [blk((height, width)), blk((height, 128))],
                [jax.ShapeDtypeStruct((vocab, width), f32), jax.ShapeDtypeStruct((vocab, 128), f32)],
                [pltpu.VMEM((cap + TOK, width), bf16), pltpu.VMEM((STAGES, CHUNK, width), f32), pltpu.SemaphoreType.DMA((STAGES,))] + z_scratch + dz_scratch,
                25_000_000_000 * (last_blk - first), {7: 0, 8: 1},
            )
        d_out_bias = jnp.sum(d_bias, axis=1)

        first_rows = pl.BlockSpec((TOK, width), lambda step, *_: (jnp.minimum(step, row_blocks - 1), 0))
        then_seqs = lambda shape: pl.BlockSpec(shape, lambda step, *_: (jnp.maximum(step - row_blocks, 0),) + (0,) * (len(shape) - 1))
        sums, d_hidden = run(
            back_kernel, (base, count.reshape(1)), row_blocks + picks, (idx_rows, d_normed, picked, w_t, vecs),
            [then_seqs((SEQS, 1, 128)), first_rows, first_rows, whole((width, width)), whole((8, width))],
            [whole((width + 8, width)), then_seqs((SEQS, seq_len, width))],
            [jax.ShapeDtypeStruct((width + 8, width), f32), jax.ShapeDtypeStruct((batch, seq_len, width), bf16)],
            [pltpu.VMEM((rows, width), f32)], 8_000_000_000,
        )
        sums = lax.psum(sums, "dp")
        d_w_t, d_b_t, d_gamma, d_beta = sums[:width], sums[width], sums[width + 1], sums[width + 2]
        return loss, d_hidden, d_w_t, d_b_t, d_gamma, d_beta, d_embed, d_out_bias

    in_specs = (P("dp", None, None), P("dp", None), P("dp", None), P("dp", None), P(None, None), P(None), P(None), P(None), P("tp", None), P("tp"))
    out_specs = (P(), P("dp", None, None), P(None, None), P(None), P(None), P(None), P("tp", None), P("tp"))
    return jax.shard_map(local_step, mesh=mesh, in_specs=in_specs, out_specs=out_specs, check_vma=False)
```

```python
import functools
import math

import jax
import jax.numpy as jnp
from jax import lax
from jax.experimental import pallas as pl
from jax.experimental.pallas import tpu as pltpu
from jax.sharding import PartitionSpec as P


LN_EPS = 1e-12
LOSS_EPS = 1e-5
SQRT_HALF = 0.5 ** 0.5
BELL_PEAK = (2.0 * math.pi) ** -0.5
VOCAB_BLOCKS = 6
TOK = 256
CHUNK = 256
STAGES = 4
PICK = 96
SEQS = 4
SPLIT = 4
OFF = 1e30
VMEM_LIMIT = 67_000_000


def normalize(pre_act):
    bell = 0.5 * (1.0 + lax.erf(pre_act * SQRT_HALF))
    activated = pre_act * bell
    centered = activated - jnp.mean(activated, axis=-1, keepdims=True)
    scale = lax.rsqrt(jnp.mean(centered * centered, axis=-1, keepdims=True) + LN_EPS)
    return centered * scale, scale, bell


def dot_nt(a, b):
    return lax.dot_general(a, b, (((1,), (1,)), ((), ())), preferred_element_type=jnp.float32)


def dot_tn(a, b):
    return lax.dot_general(a, b, (((0,), (0,)), ((), ())), preferred_element_type=jnp.float32)


def dot_nn(a, b):
    return jnp.dot(a, b, preferred_element_type=jnp.float32)


def hot_rows(row, seq_len):
    ids = lax.broadcasted_iota(jnp.int32, (seq_len, PICK), 0)
    return jnp.where(ids == row[:, :PICK], 1.0, 0.0).astype(jnp.bfloat16)


def pick_kernel(base_ref, count_ref, idx_ref, hidden_ref, weight_ref, vecs_ref, picked_ref, normed_ref, tok_ref, acc):
    step = pl.program_id(0)
    picks = base_ref.shape[0] // SEQS
    block = step - picks

    @pl.when(step == 0)
    def _():
        acc[...] = jnp.zeros_like(acc)

    @pl.when(step < picks)
    def _():
        picked = [dot_tn(hot_rows(idx_ref[k], hidden_ref.shape[1]), hidden_ref[k]) for k in range(SEQS)]
        for k, rows in enumerate(picked):
            base = pl.multiple_of(base_ref[step * SEQS + k], 8)
            acc[pl.ds(base, 16), :] += rows[:16]
            acc[pl.ds(base + 16, PICK - 16), :] = rows[16:]

    @pl.when(step >= picks)
    def _():
        rows = acc[pl.ds(pl.multiple_of(block * TOK, TOK), TOK), :].astype(jnp.bfloat16)
        picked_ref[...] = rows

        @pl.when(block * TOK < count_ref[0])
        def _():
            unit, _, _ = normalize(dot_nn(rows, weight_ref[...]) + vecs_ref[0:1, :])
            normed = unit * vecs_ref[1:2, :] + vecs_ref[2:3, :]
            normed_ref[...] = normed
            tok_ref[...] = normed.astype(jnp.bfloat16)

        @pl.when(block * TOK >= count_ref[0])
        def _():
            normed_ref[...] = jnp.zeros_like(normed_ref)
            tok_ref[...] = jnp.zeros_like(tok_ref)


def back_kernel(base_ref, count_ref, idx_ref, dnormed_ref, picked_ref, weight_ref, vecs_ref, sums_ref, dhidden_ref, drows):
    step = pl.program_id(0)
    blocks = drows.shape[0] // TOK
    width = weight_ref.shape[0]

    @pl.when(step == 0)
    def _():
        sums_ref[...] = jnp.zeros_like(sums_ref)
        drows[...] = jnp.zeros_like(drows)

    @pl.when((step < blocks) & (step * TOK < count_ref[0]))
    def _():
        pre_act = dot_nn(picked_ref[...], weight_ref[...]) + vecs_ref[0:1, :]
        unit, scale, bell = normalize(pre_act)
        dnormed = dnormed_ref[...]
        dunit = dnormed * vecs_ref[1:2, :]
        dcentered = scale * (dunit - unit * jnp.mean(dunit * unit, axis=-1, keepdims=True))
        dactivated = dcentered - jnp.mean(dcentered, axis=-1, keepdims=True)
        slope = bell + pre_act * (BELL_PEAK * jnp.exp(-0.5 * pre_act * pre_act))
        dpre = dactivated * slope
        dpre_bf = dpre.astype(jnp.bfloat16)
        sums_ref[:width, :] += dot_tn(picked_ref[...], dpre_bf)
        sums_ref[width:width + 1, :] += jnp.sum(dpre, axis=0, keepdims=True)
        sums_ref[width + 1:width + 2, :] += jnp.sum(dnormed * unit, axis=0, keepdims=True)
        sums_ref[width + 2:width + 3, :] += jnp.sum(dnormed, axis=0, keepdims=True)
        drows[pl.ds(pl.multiple_of(step * TOK, TOK), TOK), :] = dot_nt(dpre_bf, weight_ref[...])

    @pl.when(step >= blocks)
    def _():
        for k in range(SEQS):
            base = pl.multiple_of(base_ref[(step - blocks) * SEQS + k], 8)
            rows = drows[pl.ds(base, PICK), :].astype(jnp.bfloat16)
            dhidden_ref[k] = dot_nn(hot_rows(idx_ref[k], dhidden_ref.shape[1]), rows).astype(jnp.bfloat16)


def for_blocks(count, body):
    def pair(step, carry):
        body(step, 2 * TOK)
        return carry

    lax.fori_loop(0, count // 2, pair, 0)

    @pl.when(count % 2 == 1)
    def _():
        body(count // 2, TOK)


def strips(height):
    size = height // 4 // 256 * 256
    return [(k * size, size if k < 3 else height - 3 * size) for k in range(4)]


def tile_bias(bias_ref, at, size, width):
    bias = bias_ref[at:at + size, :]
    return jnp.concatenate([bias] * (width // bias.shape[1]), axis=1)


def stats_kernel(count_ref, lab_ref, tok_ref, embed_ref, bias_ref, out_ref, logits_hbm, z_ref, sems):
    vblk = pl.program_id(0)
    height = embed_ref.shape[0]
    steps = (count_ref[0] + 1) // 2

    def save(vocab_blk, step, slot):
        return pltpu.make_async_copy(z_ref.at[slot], logits_hbm.at[vocab_blk, step], sems.at[slot])

    @pl.when(vblk == 0)
    def _():
        out_ref[...] = jnp.zeros_like(out_ref)
        out_ref[0:1, :] = jnp.full((1, out_ref.shape[1]), -jnp.inf, jnp.float32)

    def body(step, width):
        cols = pl.ds(pl.multiple_of(step * 2 * TOK, 2 * TOK), width)
        turn = vblk * steps + step
        slot = lax.rem(turn, 2)

        @pl.when(turn >= 2)
        def _():
            save(vblk, step, slot).wait()

        tok = tok_ref[cols, :]
        lab = lab_ref[0:1, cols] - vblk * height
        parts = []
        target = jnp.zeros((1, width), jnp.float32)
        todo = strips(height)

        def logits(at, size):
            z_ref[slot, at:at + size, :width] = dot_nt(embed_ref[at:at + size, :], tok) + tile_bias(bias_ref, at, size, width)

        logits(*todo[0])
        for k, (at, size) in enumerate(todo):
            if k + 1 < len(todo):
                logits(*todo[k + 1])
            z = z_ref[slot, at:at + size, :width]
            top = jnp.max(z, axis=0, keepdims=True)
            total = jnp.sum(jnp.exp(z - top), axis=0, keepdims=True)
            hit = lax.broadcasted_iota(jnp.int32, (size, width), 0) == lab - at
            target += jnp.sum(jnp.where(hit, z, 0.0), axis=0, keepdims=True)
            parts.append((top, total))
        old_max = out_ref[0:1, cols]
        new_max = functools.reduce(jnp.maximum, [top for top, _ in parts], old_max)
        total = out_ref[1:2, cols] * jnp.exp(old_max - new_max)
        for top, part in parts:
            total += part * jnp.exp(top - new_max)
        out_ref[0:1, cols] = new_max
        out_ref[1:2, cols] = total
        out_ref[2:3, cols] += target
        save(vblk, step, slot).start()

    for_blocks(count_ref[0], body)

    @pl.when(vblk == pl.num_programs(0) - 1)
    def _():
        turns = pl.num_programs(0) * steps
        save(0, 0, lax.rem(turns, 2)).wait()
        save(0, 0, lax.rem(turns + 1, 2)).wait()


def grad_strip(at, size, width, z, lab, top, scale, unit, dbias_ref, dz_ref, fresh=None):
    lanes = dbias_ref.shape[1]
    hit = lax.broadcasted_iota(jnp.int32, (size, width), 0) == lab - at
    dz = jnp.exp(z - top) * scale - jnp.where(hit, unit, 0.0)
    part = dz[:, :lanes]
    for j in range(1, width // lanes):
        part = part + dz[:, j * lanes:(j + 1) * lanes]
    old = dbias_ref[at:at + size, :]
    dbias_ref[at:at + size, :] = part + (old if fresh is None else jnp.where(fresh, 0.0, old))
    dz_ref[at:at + size, :width] = dz.astype(jnp.bfloat16)


def token_row(cols, vblk, height, lab_ref, meta_ref):
    return lab_ref[0:1, cols] - vblk * height, meta_ref[0:1, cols], meta_ref[1:2, cols], meta_ref[2:3, cols]


def own_kernel(count_ref, lab_ref, meta_ref, tok_ref, embed_ref, logits_hbm, dembed_ref, dbias_ref, dtok_ref, z_ref, sems, dz_ref):
    vblk = pl.program_id(0)
    height = embed_ref.shape[0]
    steps = (count_ref[0] + 1) // 2

    def load(vocab_blk, step, slot):
        return pltpu.make_async_copy(logits_hbm.at[vocab_blk, step], z_ref.at[slot], sems.at[slot])

    @pl.when(vblk == 0)
    def _():
        dtok_ref[...] = jnp.zeros_like(dtok_ref)
        load(0, 0, 0).start()

    def body(step, width):
        turn = vblk * steps + step
        slot = lax.rem(turn, 2)
        wrap = step + 1 == steps
        next_blk, next_step = jnp.where(wrap, vblk + 1, vblk), jnp.where(wrap, 0, step + 1)

        @pl.when(next_blk < pl.num_programs(0))
        def _():
            load(next_blk, next_step, 1 - slot).start()

        load(vblk, step, slot).wait()
        cols = pl.ds(pl.multiple_of(step * 2 * TOK, 2 * TOK), width)
        tok = tok_ref[cols, :]
        row = token_row(cols, vblk, height, lab_ref, meta_ref)
        fresh = step == 0
        todo = strips(height)

        def grad(at, size):
            grad_strip(at, size, width, z_ref[slot, at:at + size, :width], *row, dbias_ref, dz_ref, fresh)

        grad(*todo[0])
        for k, (at, size) in enumerate(todo):
            if k + 1 < len(todo):
                grad(*todo[k + 1])
            dz = dz_ref[at:at + size, :width]
            dembed_ref[at:at + size, :] = dot_nn(dz, tok) + jnp.where(fresh, 0.0, dembed_ref[at:at + size, :])
            dtok_ref[cols, :] += dot_tn(dz, embed_ref[at:at + size, :])

    for_blocks(count_ref[0], body)


def rest_kernel(first, plan_ref, src_ref, dst_ref, lab_ref, meta_ref, embed_ref, bias_ref, dembed_in_ref, dbias_in_ref, tok_hbm, dembed_ref, dbias_ref, tok_ref, stage, sems, z_ref, dz_ref):
    vblk = pl.program_id(0)
    chunks = plan_ref[1]

    def fetch(chunk):
        slot = lax.rem(chunk, STAGES)
        src = tok_hbm.at[pl.ds(pl.multiple_of(src_ref[chunk], CHUNK), CHUNK), :]
        return pltpu.make_async_copy(src, stage.at[slot], sems.at[slot])

    @pl.when(vblk == 0)
    def _():
        end = pl.multiple_of(plan_ref[2], 16)
        tok_ref[pl.ds(end, TOK), :] = jnp.zeros((TOK, tok_ref.shape[1]), jnp.bfloat16)
        for k in range(STAGES):
            @pl.when(k < chunks)
            def _():
                fetch(k).start()

        def take(chunk, carry):
            fetch(chunk).wait()
            dst = pl.multiple_of(dst_ref[chunk], 16)
            tok_ref[pl.ds(dst, CHUNK), :] = stage[lax.rem(chunk, STAGES)].astype(jnp.bfloat16)

            @pl.when(chunk + STAGES < chunks)
            def _():
                fetch(chunk + STAGES).start()

            return carry

        lax.fori_loop(0, chunks, take, 0)

    dembed_ref[...] = dembed_in_ref[...]
    dbias_ref[...] = dbias_in_ref[...]

    height = embed_ref.shape[0]

    def body(step, width):
        cols = pl.ds(pl.multiple_of(step * 2 * TOK, 2 * TOK), width)
        tok = tok_ref[cols, :]
        row = token_row(cols, vblk + first, height, lab_ref, meta_ref)
        todo = strips(height)

        def logits(at, size):
            z_ref[at:at + size, :width] = dot_nt(embed_ref[at:at + size, :], tok)

        logits(*todo[0])
        for k, (at, size) in enumerate(todo):
            if k + 1 < len(todo):
                logits(*todo[k + 1])
            grad_strip(at, size, width, z_ref[at:at + size, :width] + tile_bias(bias_ref, at, size, width), *row, dbias_ref, dz_ref)
            dembed_ref[at:at + size, :] += dot_nn(dz_ref[at:at + size, :width], tok)

    for_blocks(plan_ref[0], body)


def whole(shape):
    return pl.BlockSpec(shape, lambda *_: (0,) * len(shape))


def by_rows(shape, first=0):
    return pl.BlockSpec(shape, lambda step, *_: (step + first,) + (0,) * (len(shape) - 1))


def run(kernel, scalars, grid, args, in_specs, out_specs, out_shape, scratch, flops, aliases=None):
    return pl.pallas_call(
        kernel,
        grid_spec=pltpu.PrefetchScalarGridSpec(
            num_scalar_prefetch=len(scalars), grid=(grid,), in_specs=in_specs, out_specs=out_specs, scratch_shapes=scratch
        ),
        out_shape=out_shape,
        input_output_aliases=aliases or {},
        compiler_params=pltpu.CompilerParams(dimension_semantics=("arbitrary",), vmem_limit_bytes=VMEM_LIMIT),
        cost_estimate=pl.CostEstimate(flops=flops, bytes_accessed=40_000_000, transcendentals=0),
    )(*scalars, *args)


def solution(mesh):
    groups, shards = mesh.shape["dp"], mesh.shape["tp"]
    f32, bf16, i32 = jnp.float32, jnp.bfloat16, jnp.int32

    def local_step(hidden, positions, labels, weights, w_t, b_t, gamma, beta, embed, out_bias):
        batch, seq_len, width = hidden.shape
        max_pred = positions.shape[1]
        rows = batch * max_pred
        vocab = embed.shape[0]
        height = vocab // VOCAB_BLOCKS
        me_dp, me_tp = lax.axis_index("dp"), lax.axis_index("tp")

        live = jnp.sum(weights, axis=1).astype(i32)
        seqs = jnp.arange(batch, dtype=i32)
        offset = jnp.sum(jnp.where(seqs[None, :] < seqs[:, None], live[None, :], 0), axis=1)
        base = jnp.minimum(offset // 8 * 8, rows - PICK)
        slots = jnp.arange(max_pred, dtype=i32)
        alive = slots[None, :] < live[:, None]
        place = jnp.where(alive, slots[None, :] + (offset - base)[:, None], -1)
        lanes = jnp.arange(128, dtype=i32)
        idx_rows = jnp.sum(jnp.where(place[:, None, :] == lanes[None, :, None], positions[:, None, :] + 1, 0), axis=2) - 1
        idx_rows = idx_rows.reshape(batch, 1, 128)
        packed = jnp.where(alive, slots[None, :] + offset[:, None], -1).reshape(-1)
        lab = jnp.sum(jnp.where(packed[None, :] == jnp.arange(rows, dtype=i32)[:, None], labels.reshape(-1)[None, :] + 1, 0), axis=1) - 1
        count = jnp.sum(live)
        blocks = ((count + TOK - 1) // TOK).reshape(1)

        picks, row_blocks = batch // SEQS, rows // TOK
        vecs = jnp.stack([b_t, gamma, beta] + [jnp.zeros_like(b_t)] * 5)
        early = lambda shape: pl.BlockSpec(shape, lambda step, *_: (jnp.minimum(step, picks - 1),) + (0,) * (len(shape) - 1))
        late = pl.BlockSpec((TOK, width), lambda step, *_: (jnp.maximum(step - picks, 0), 0))
        picked, normed, tok = run(
            pick_kernel, (base, count.reshape(1)), picks + row_blocks, (idx_rows, hidden, w_t, vecs),
            [early((SEQS, 1, 128)), early((SEQS, seq_len, width)), whole((width, width)), whole((8, width))], [late] * 3,
            [jax.ShapeDtypeStruct((rows, width), bf16), jax.ShapeDtypeStruct((rows, width), f32), jax.ShapeDtypeStruct((rows, width), bf16)],
            [pltpu.VMEM((rows, width), f32)], 8_000_000_000,
        )
        share = rows // shards
        mine = lax.dynamic_slice(normed, (me_tp * share, 0), (share, width))
        tok_all = lax.all_gather(mine, ("dp", "tp"), tiled=True)

        bias = jnp.broadcast_to(out_bias[:, None], (vocab, 128))
        local_lab = jnp.where(lab >= 0, lab - me_tp * vocab, -1)
        z_scratch = [pltpu.VMEM((height, 2 * TOK), f32)]
        dz_scratch = [pltpu.VMEM((height, 2 * TOK), bf16)]
        logit_shape = (VOCAB_BLOCKS, -(-rows // (2 * TOK)), height, 2 * TOK)
        slots_scratch = [pltpu.VMEM((2, height, 2 * TOK), f32), pltpu.SemaphoreType.DMA((2,))]
        anywhere = pl.BlockSpec(memory_space=pl.ANY)
        stats, logits = run(
            stats_kernel, (blocks,), VOCAB_BLOCKS, (local_lab[None, :], tok, embed, bias),
            [whole((1, rows)), whole((rows, width)), by_rows((height, width)), by_rows((height, 128))], [whole((8, rows)), anywhere],
            [jax.ShapeDtypeStruct((8, rows), f32), jax.ShapeDtypeStruct(logit_shape, f32)], slots_scratch, 25_000_000_000,
        )
        packet = jnp.concatenate([stats[:3], lab.astype(f32)[None, :]], axis=0)
        packets = lax.all_gather(packet, ("dp", "tp")).reshape(groups, shards, 4, rows)
        labs = packets[:, 0, 3, :].astype(i32)
        valid = labs >= 0
        maxes = jnp.where(valid[:, None, :], packets[:, :, 0, :], 0.0)
        row_max = jnp.max(maxes, axis=1)
        sum_exp = jnp.where(valid, jnp.sum(packets[:, :, 1, :] * jnp.exp(maxes - row_max[:, None, :]), axis=1), 1.0)
        target = jnp.sum(packets[:, :, 2, :], axis=1)
        lives = jnp.sum(valid, axis=1).astype(i32)
        denom = jnp.sum(lives).astype(f32) + LOSS_EPS
        loss = jnp.sum(jnp.where(valid, jnp.log(sum_exp) + row_max - target, 0.0)) / denom
        inv = 1.0 / denom
        metas = jnp.stack([
            jnp.where(valid, row_max, OFF),
            jnp.where(valid, (1.0 / sum_exp) * inv, 0.0),
            jnp.where(valid, inv, 0.0),
            jnp.where(valid, labs - me_tp * vocab, -1).astype(f32),
        ], axis=1)

        own_meta = lax.dynamic_index_in_dim(metas, me_dp, 0, keepdims=False)
        d_embed, d_bias_own, d_tok = run(
            own_kernel, (blocks,), VOCAB_BLOCKS, (local_lab[None, :], own_meta, tok, embed, logits),
            [whole((1, rows)), whole((4, rows)), whole((rows, width)), by_rows((height, width)), anywhere],
            [by_rows((height, width)), by_rows((height, 128)), whole((rows, width))],
            [jax.ShapeDtypeStruct((vocab, width), f32), jax.ShapeDtypeStruct((vocab, 128), f32), jax.ShapeDtypeStruct((rows, width), f32)],
            slots_scratch + dz_scratch, 50_000_000_000,
        )
        d_normed = lax.psum(d_tok, "tp")

        cap = (groups - 1) * rows
        meta = jnp.concatenate([jnp.full((1, cap + TOK), OFF, f32), jnp.zeros((2, cap + TOK), f32), jnp.full((1, cap + TOK), -1.0, f32)], axis=0)
        pos = jnp.int32(0)
        ids = jnp.arange(cap // CHUNK, dtype=i32)
        src, dst, chunks = jnp.zeros_like(ids), jnp.zeros_like(ids), jnp.int32(0)
        for k in range(1, groups):
            peer = lax.rem(me_dp + k, groups)
            meta = lax.dynamic_update_slice(meta, lax.dynamic_index_in_dim(metas, peer, 0, keepdims=False), (0, pos))
            size = lax.dynamic_index_in_dim(lives, peer, 0, keepdims=False)
            parts = (size + CHUNK - 1) // CHUNK
            inside = ids >= chunks
            src = jnp.where(inside, peer * rows + (ids - chunks) * CHUNK, src)
            dst = jnp.where(inside, pos + (ids - chunks) * CHUNK, dst)
            chunks = chunks + parts
            last = pos + parts * CHUNK
            pos = pos + (size + 15) // 16 * 16
        plan = jnp.stack([(pos + TOK - 1) // TOK, chunks, last])
        meta_lab = meta[3:4].astype(i32)
        d_bias = d_bias_own
        for first, last_blk in ((0, SPLIT), (SPLIT, VOCAB_BLOCKS)):
            blk = functools.partial(by_rows, first=first)
            d_embed, d_bias = run(
                functools.partial(rest_kernel, first), (plan, src, dst), last_blk - first, (meta_lab, meta, embed, bias, d_embed, d_bias, tok_all),
                [whole((1, cap + TOK)), whole((4, cap + TOK)), blk((height, width)), blk((height, 128)), blk((height, width)), blk((height, 128)), pl.BlockSpec(memory_space=pl.ANY)],
                [blk((height, width)), blk((height, 128))],
                [jax.ShapeDtypeStruct((vocab, width), f32), jax.ShapeDtypeStruct((vocab, 128), f32)],
                [pltpu.VMEM((cap + TOK, width), bf16), pltpu.VMEM((STAGES, CHUNK, width), f32), pltpu.SemaphoreType.DMA((STAGES,))] + z_scratch + dz_scratch,
                25_000_000_000 * (last_blk - first), {7: 0, 8: 1},
            )
        d_out_bias = jnp.sum(d_bias, axis=1)

        first_rows = pl.BlockSpec((TOK, width), lambda step, *_: (jnp.minimum(step, row_blocks - 1), 0))
        then_seqs = lambda shape: pl.BlockSpec(shape, lambda step, *_: (jnp.maximum(step - row_blocks, 0),) + (0,) * (len(shape) - 1))
        sums, d_hidden = run(
            back_kernel, (base, count.reshape(1)), row_blocks + picks, (idx_rows, d_normed, picked, w_t, vecs),
            [then_seqs((SEQS, 1, 128)), first_rows, first_rows, whole((width, width)), whole((8, width))],
            [whole((width + 8, width)), then_seqs((SEQS, seq_len, width))],
            [jax.ShapeDtypeStruct((width + 8, width), f32), jax.ShapeDtypeStruct((batch, seq_len, width), bf16)],
            [pltpu.VMEM((rows, width), f32)], 8_000_000_000,
        )
        sums = lax.psum(sums, "dp")
        d_w_t, d_b_t, d_gamma, d_beta = sums[:width], sums[width], sums[width + 1], sums[width + 2]
        return loss, d_hidden, d_w_t, d_b_t, d_gamma, d_beta, d_embed, d_out_bias

    in_specs = (P("dp", None, None), P("dp", None), P("dp", None), P("dp", None), P(None, None), P(None), P(None), P(None), P("tp", None), P("tp"))
    out_specs = (P(), P("dp", None, None), P(None, None), P(None), P(None), P(None), P("tp", None), P("tp"))
    return jax.shard_map(local_step, mesh=mesh, in_specs=in_specs, out_specs=out_specs, check_vma=False)
```
